32 devices in a mesh: scene: 2 (over y), pulse: 4 (over z), rng: 2 (over core), pol: 2 (over x).
Axes of the slice: x: 2, y: 2, z: 4, core: 2. Of those that a mesh axis runs over, the one named last changes fastest.
Arguments:
- echoes: bfloat16 [8, 2, 128, 8192], P(('scene', 'pol'), None, None, ('pulse', 'rng')), parts along dimension 0, may hold values from -6 to 6
- migration: int32 [32, 8192], P(('scene', 'pulse', 'rng')), parts along dimension 0, may hold values from 0 to 8
- fm_rate: float32 [256], P(('scene', 'pulse', 'rng')), parts along dimension 0, may hold values from 0.05 to 0.2
Outputs:
- coherency: bfloat16 [9, 256, 8192], P(None, ('scene', 'pulse', 'rng'), 'pol'), parts along dimension 1
The draws below stay inside these ranges and needn't reach their ends.
There are 2 independent parts, one for each index of `scene`. The reference program is written for one: setup_inputs(seed, part) draws one part's arguments, and reference() takes and returns one part's arrays. A program takes and returns all parts, laid end to end along the dimension named above; each array names one. Nothing has to cross between parts.
Inputs may be any that keep to these rules, and one draw needn't show every extreme that they name: migration[b, f] is the shift in bins for range bins b * 8 to (b + 1) * 8 - 1 at azimuth frequency bin f.
All inputs are finite; a program needn't handle non-finite values.
Results may differ from the reference program's by a relative error of at most 0.006.
Values may be sent and summed in bfloat16 or wider, within the bound.
A program may use at most 64 MiB of HBM per device.

```python
import math
import jax
import jax.numpy as jnp
from jax import lax

P_SIZE = 8192
R = 128
RBLK = 8
RANGE_BLOCKS = 16
SMAX = 8
WIN = 7


def set_ends(values, key, low, top_value):
    longest = values.shape.index(max(values.shape))
    spots = []
    for shift in (0, 1):
        where = [jax.random.randint(jax.random.fold_in(key, axis), (), 0, length) for axis, length in enumerate(values.shape)]
        where[longest] = (where[longest] + shift) % values.shape[longest]
        spots.append(tuple(where))
    return values.at[spots[0]].set(low).at[spots[1]].set(top_value)


def levels(own_key, dims, pieces, smallest, high):
    loudness, own = 1.0, jax.random.fold_in(own_key, 6)
    for axis_at, shards_of in pieces:
        steps = jnp.exp(jax.random.uniform(jax.random.fold_in(own, axis_at), (shards_of,), jnp.float32, smallest / len(pieces), high / len(pieces)))
        loudness = loudness * jnp.repeat(steps, dims[axis_at] // shards_of).reshape([-1 if axis == axis_at else 1 for axis in range(len(dims))])
    return loudness


def gaussian(rng, extent, spread, reach, shards=(), kind=jnp.bfloat16):
    array = spread * jax.random.normal(rng, extent, jnp.float32)
    if shards:
        array = array * levels(rng, extent, shards, -0.22, 0.18)
    return jnp.clip(array, -reach, reach).astype(kind)


def setup_inputs(seed: int = 0, part: int = 0) -> dict:
    streams_of = jax.random.split(jax.random.key(seed), 4)
    part_splits = jax.random.split(jax.random.fold_in(streams_of[3], part), 4)
    return {
        "echoes": gaussian(part_splits[0], (4, 2, R, P_SIZE), 1.0, 6.0, ((0, 2), (3, 8))),
        "migration": set_ends(jax.random.randint(part_splits[1], (RANGE_BLOCKS, P_SIZE), 0, SMAX + 1), jax.random.fold_in(part_splits[1], 1), 0, SMAX).astype(jnp.int32),
        "fm_rate": jnp.clip(jnp.exp(math.log(0.2) - 1.3862944 * jax.random.uniform(part_splits[2], (R,), jnp.float32) ** levels(part_splits[2], (R,), ((0, 8),), -0.2, 0.2)), 0.05, 0.2),
    }


root_half = 0.7071067811865476


def squared(vector):
    return vector[0] * vector[0] + vector[1] * vector[1]


def cross_term(first, second):
    return first[0] * second[0] + first[1] * second[1], first[1] * second[0] - first[0] * second[1]


def pauli_terms(channel):
    values = channel.astype(jnp.float32)
    first = (values[0] + values[3]) * root_half
    second = (values[0] - values[3]) * root_half
    third = (values[1] + values[2]) * root_half
    one_two = cross_term(first, second)
    one_three = cross_term(first, third)
    two_three = cross_term(second, third)
    return [squared(first), squared(second), squared(third), one_two[0], one_two[1], one_three[0], one_three[1], two_three[0], two_three[1]]


def focus(channel, migration, fm_rate):
    signal = channel[0].astype(jnp.float32) + 1j * channel[1].astype(jnp.float32)
    spectrum = jnp.fft.fft(signal, axis=-1, norm="ortho")
    parts = jnp.stack([spectrum.real, spectrum.imag]).astype(jnp.bfloat16)
    parts = jnp.pad(parts, ((0, 0), (0, SMAX), (0, 0)))
    offsets = lax.broadcasted_iota(jnp.int32, (R, P_SIZE), 0) + jnp.repeat(migration, RBLK, axis=0)
    moved = jnp.take_along_axis(parts, jnp.broadcast_to(offsets[None], (2, R, P_SIZE)), axis=1).astype(jnp.float32)
    frequency = jnp.arange(P_SIZE, dtype=jnp.int32)
    centred = jnp.where(frequency < P_SIZE // 2, frequency, frequency - P_SIZE).astype(jnp.float32)
    phase = (jnp.pi * fm_rate[:, None]) * (centred * centred / P_SIZE)
    cosine = jnp.cos(phase)
    sine = jnp.sin(phase)
    comp_real = moved[0] * cosine - moved[1] * sine
    comp_imag = moved[0] * sine + moved[1] * cosine
    image = jnp.fft.ifft(comp_real + 1j * comp_imag, axis=-1, norm="ortho")
    return jnp.stack([image.real, image.imag]).astype(jnp.bfloat16)


def window_average(component):
    half = WIN // 2
    padded = jnp.pad(component, half)
    along = padded[0:R, :]
    for offset in range(1, WIN):
        along = along + padded[offset:offset + R, :]
    totals = along[:, 0:P_SIZE]
    for offset in range(1, WIN):
        totals = totals + along[:, offset:offset + P_SIZE]
    return (totals / (WIN * WIN)).astype(jnp.bfloat16)


def reference(echoes, migration, fm_rate):
    image = lax.map(lambda channel: focus(channel, migration, fm_rate), echoes)
    terms = pauli_terms(image)
    return jnp.stack([window_average(component) for component in terms])
```

```python
import functools
import math

import jax
import jax.numpy as jnp
import numpy as np
from jax import lax
from jax.experimental import pallas as pl
from jax.experimental.pallas import tpu as pltpu
from jax.sharding import PartitionSpec as P

RBLK = 8
SMAX = 8
WIN = 7
HALF = WIN // 2
LANES = 128
STEP = 4
SLOTS = 3
AHEAD = 3
LAG = 1
FIRST = 0
RAW = 1
DRAIN = AHEAD + LAG + FIRST
ROOT_HALF = 0.7071067811865476
MESH = pl.DeviceIdType.MESH
F32 = jnp.float32
BF16 = jnp.bfloat16


def fit(function, degree):
    nodes = (np.cos(np.pi * (np.arange(64) + 0.5) / 64) + 1) / 8
    poly = np.polynomial.Chebyshev.fit(nodes, function(nodes), degree, domain=[0, 0.25])
    return [float(v) for v in poly.convert(kind=np.polynomial.Polynomial).coef]


SIN_COEF = fit(lambda y: np.sin(2 * np.pi * np.sqrt(y)) / np.sqrt(y), 7)
COS_COEF = fit(lambda y: np.cos(2 * np.pi * np.sqrt(y)), 7)


def horner(coefs, y):
    total = jnp.full_like(y, coefs[-1])
    for coef in coefs[-2::-1]:
        total = total * y + coef
    return total


def trig(period, height, width):
    index = np.arange(height)[:, None] * np.arange(width)[None, :] % period
    return np.cos(2 * np.pi * index / period), np.sin(2 * np.pi * index / period)


def tables(outer):
    size = outer * LANES
    oc, os_ = trig(outer, outer, outer)
    scale = 1.0 / math.sqrt(outer)
    first = np.block([[oc, os_], [-os_, oc]]) * scale
    last = np.block([[oc, -os_], [os_, oc]]) * scale
    ic, is_ = trig(LANES, LANES, LANES)
    fwd = np.block([[ic, -is_], [is_, ic]])
    inv = np.block([[ic, is_], [-is_, ic]])
    tc, ts = trig(size, outer, LANES)
    row = np.arange(LANES)
    gap = row[:, None] - row[None, :]
    near = np.abs(gap) <= HALF
    wrap = np.abs(np.abs(gap) - LANES) <= HALF
    band = np.concatenate([near, wrap], axis=0)
    per_row = LANES // outer
    spread = np.zeros((per_row * outer, LANES))
    for u in range(outer):
        for h in range(per_row):
            spread[h * outer + u, per_row * u + h] = 1
    short = lambda v: np.asarray(v, np.float32).astype(BF16).astype(np.float32)

    def gain(v):
        return float(np.sum(v * short(v)) / np.sum(v * v))

    root = math.sqrt(LANES)
    there, back = root * gain(first) * gain(fwd), root * gain(inv) * gain(last)
    twiddle = np.stack([tc / there, ts / there, tc / back, ts / back])
    fill = lambda v, width: np.pad(v, ((0, 0), (0, width - v.shape[1])))
    slim = np.concatenate([fill(first, LANES), fill(last, LANES), spread])
    wide = np.concatenate([fwd, inv, fill(band, 2 * LANES)])
    return jnp.asarray(wide, BF16), jnp.asarray(slim, BF16), jnp.asarray(twiddle, F32)


def kernel(
    chans, groups, pols, bins, outer, rng_size,
    echo, mig_hbm, rate, wide_hbm, slim_hbm, twiddle_hbm,
    out,
    mig, wide_t, slim_t, twiddle, t_sem,
    recv, unpacked, spec, image, edge, quad, quad_edge, shifts, mig_rows, cosine, sine,
    cells, cells_edge, padded, result,
    z_send, z_recv, h_send, h_recv, x_send, x_recv, e_send, e_recv, r_send, r_recv, f_send, f_recv,
):
    half_rows = outer // pols
    local_a = outer // groups
    pulse_i, rng_i, pol_i = (lax.axis_index(n) for n in ("pulse", "rng", "pol"))
    me = pulse_i * rng_size + rng_i

    def member(q):
        return {"pulse": q // rng_size, "rng": lax.rem(q, rng_size)}

    fetches = [
        pltpu.make_async_copy(source, target, t_sem.at[i])
        for i, (source, target) in enumerate(
            ((mig_hbm, mig), (slim_hbm, slim_t), (twiddle_hbm, twiddle), (wide_hbm, wide_t))
        )
    ]
    for fetch in fetches:
        fetch.start()
    two = 2 * outer
    first_t, last_t = slim_t.at[0:two, 0:two], slim_t.at[two : 2 * two, 0:two]
    fwd_t, inv_t = wide_t.at[0 : 2 * LANES], wide_t.at[2 * LANES : 4 * LANES]
    band = wide_t.at[4 * LANES : 6 * LANES, 0:LANES]

    barrier = pltpu.get_barrier_semaphore()

    def greet_group(k, carry):
        pl.semaphore_signal(
            barrier, inc=1, device_id=member(lax.rem(me + k, groups)), device_id_type=MESH
        )
        return carry

    lax.fori_loop(1, groups, greet_group, 0)
    for k in range(1, pols):
        pl.semaphore_signal(
            barrier, inc=1, device_id={"pol": lax.rem(pol_i + k, pols)}, device_id_type=MESH
        )
    pl.semaphore_wait(barrier, groups - 1 + pols - 1)

    depth = groups // rng_size
    quads = bins // STEP
    halos = SMAX // STEP
    units = chans * quads
    mid = rng_size * (depth // 2)

    def z_copy(unit, first, slot, q):
        ch, part = unit // quads, lax.rem(unit, quads)
        start = pl.multiple_of(first * bins + part * STEP, STEP)
        return pltpu.make_async_remote_copy(
            src_ref=echo.at[ch, :, pl.ds(start, STEP), :],
            dst_ref=recv.at[slot, me],
            send_sem=z_send.at[slot],
            recv_sem=z_recv.at[slot],
            device_id=member(q),
            device_id_type=MESH,
        )

    def own_copy(unit, first, slot):
        ch, part = unit // quads, lax.rem(unit, quads)
        start = pl.multiple_of(first * bins + part * STEP, STEP)
        return pltpu.make_async_copy(
            echo.at[ch, :, pl.ds(start, STEP), :], recv.at[slot, me], z_recv.at[slot]
        )

    def z_landed(slot):
        pltpu.make_async_copy(recv.at[slot], recv.at[slot], z_recv.at[slot]).wait()

    def z_sent(slot):
        some = recv.at[slot, pl.ds(0, groups - 1)]
        pltpu.make_async_copy(some, some, z_send.at[slot]).wait()

    def send_step(step):
        def to_layer(layer, near):
            for j in range(rng_size):
                q = layer * rng_size + j
                unit = step - LAG * j - FIRST * jnp.minimum(layer, 1)
                valid = (unit >= 0) & (unit < units)
                if near:

                    @pl.when(valid & (rng_i == j))
                    def _():
                        own_copy(unit, me, unit).start()

                    valid = valid & (rng_i != j)

                @pl.when(valid)
                def _():
                    z_copy(unit, q, unit, q).start()

        def send_echo(i, carry):
            gap = depth - 1 - i
            for sign in (1, -1):
                layer = pulse_i + sign * gap

                @pl.when((layer >= 0) & (layer < depth))
                def _(layer=layer):
                    to_layer(layer, False)

            return carry

        lax.fori_loop(0, depth - 1, send_echo, 0)
        to_layer(pulse_i, True)
        early = step - LAG - FIRST - RAW
        slot = units + early // quads * halos + lax.rem(early, quads)
        valid = (early >= 0) & (early < units) & (lax.rem(early, quads) < halos)
        if mid > 0:

            @pl.when(valid & (me == mid - 1))
            def _():
                own_copy(early, mid, slot).start()

            @pl.when(valid & (me != mid - 1))
            def _():
                z_copy(early, mid, slot, mid - 1).start()

    mylag = LAG * rng_i + FIRST * jnp.minimum(pulse_i, 1)

    def opening(step, carry):
        send_step(step)
        return carry

    lax.fori_loop(0, AHEAD + mylag, opening, 0)

    def zero_edges():
        @pl.when(me == groups - 1)
        def _():
            spec[:, :, bins:, :, :] = jnp.zeros((chans, 2, SMAX, outer, LANES), BF16)
            quad[:, :, HALF + bins :, :, :] = jnp.zeros((4, 2, HALF, half_rows, LANES), BF16)
            quad_edge[:, :, HALF + bins :, :, :] = jnp.zeros((4, 2, HALF, 2, LANES), F32)

        @pl.when(me == 0)
        def _():
            quad[:, :, :HALF, :, :] = jnp.zeros((4, 2, HALF, half_rows, LANES), BF16)
            quad_edge[:, :, :HALF, :, :] = jnp.zeros((4, 2, HALF, 2, LANES), F32)

    zero_edges()
    for fetch in fetches:
        fetch.wait()

    per_row = LANES // outer
    for k in range(mig.shape[0]):
        for u in range(outer):
            mig_rows[u : u + 1, :] = mig[k : k + 1, u * LANES : (u + 1) * LANES].astype(F32)
        turned = mig_rows[...].T.astype(BF16)
        total = jnp.zeros((outer, LANES), F32)
        for h in range(per_row):
            total = total + jnp.dot(
                turned[h * outer : (h + 1) * outer],
                slim_t[(2 * two + h * outer) : (2 * two + (h + 1) * outer)],
                preferred_element_type=F32,
            )
        shifts[k] = total.astype(BF16)

    size = outer * LANES
    position = lax.broadcasted_iota(jnp.int32, (outer, LANES), 0) + outer * (
        lax.broadcasted_iota(jnp.int32, (outer, LANES), 1)
    )
    centred = jnp.where(position < size // 2, position, position - size).astype(F32)
    quadratic = centred * centred / size

    def phase_row(r, carry):
        turns = (0.5 * rate[r]) * quadratic
        turns = turns - jnp.round(turns)
        square = turns * turns
        cosine[r] = horner(COS_COEF, square)
        sine[r] = horner(SIN_COEF, square) * turns
        return carry

    lax.fori_loop(0, bins, phase_row, 0)

    def halo_copy(ch, part):
        return pltpu.make_async_remote_copy(
            src_ref=spec.at[ch, :, pl.ds(part * STEP, STEP)],
            dst_ref=spec.at[ch, :, pl.ds(bins + part * STEP, STEP)],
            send_sem=h_send.at[ch, part],
            recv_sem=h_recv.at[ch, part],
            device_id=member(jnp.maximum(me - 1, 0)),
            device_id_type=MESH,
        )

    def x_copy(ch, blk, k):
        return pltpu.make_async_remote_copy(
            src_ref=image.at[ch, k - 1, :, pl.ds(blk * STEP, STEP)],
            dst_ref=quad.at[pol_i * chans + ch, :, pl.ds(HALF + blk * STEP, STEP)],
            send_sem=x_send.at[ch],
            recv_sem=x_recv.at[ch, blk],
            device_id={"pol": lax.rem(pol_i + k, pols)},
            device_id_type=MESH,
        )

    def e_copy(ch, blk, k):
        return pltpu.make_async_remote_copy(
            src_ref=edge.at[ch, k - 1, :, pl.ds(blk * STEP, STEP)],
            dst_ref=quad_edge.at[pol_i * chans + ch, :, pl.ds(HALF + blk * STEP, STEP)],
            send_sem=e_send.at[ch],
            recv_sem=e_recv.at[ch, blk],
            device_id={"pol": lax.rem(pol_i + k, pols)},
            device_id_type=MESH,
        )

    def landed(ch, blk):
        if pols > 1:
            rows = pl.ds(HALF + blk * STEP, STEP)
            some = quad.at[pl.ds(0, pols - 1), :, rows]
            few = quad_edge.at[pl.ds(0, pols - 1), :, rows]
            pltpu.make_async_copy(some, some, x_recv.at[ch, blk]).wait()
            pltpu.make_async_copy(few, few, e_recv.at[ch, blk]).wait()

    def x_sent(ch):
        if pols > 1:
            some, few = image.at[ch], edge.at[ch]
            pltpu.make_async_copy(some, some, x_send.at[ch]).wait()
            pltpu.make_async_copy(few, few, e_send.at[ch]).wait()

    def relay(array, sems, recvs, chan, side):
        take = HALF if side == 0 else bins
        put = HALF + bins if side == 0 else 0
        target = jnp.maximum(me - 1, 0) if side == 0 else jnp.minimum(me + 1, groups - 1)
        return pltpu.make_async_remote_copy(
            src_ref=array.at[chan, :, pl.ds(take, HALF)],
            dst_ref=array.at[chan, :, pl.ds(put, HALF)],
            send_sem=sems.at[side],
            recv_sem=recvs.at[side],
            device_id=member(target),
            device_id_type=MESH,
        )

    sides = ((0, me > 0), (1, me < groups - 1))

    def relayed(array, sems):
        rows = array.at[:, :, pl.ds(0, HALF)]
        for side, cond in sides:

            @pl.when(cond)
            def _(side=side):
                pltpu.make_async_copy(rows, rows, sems.at[side]).wait()

    def unpack(slot):
        def body(p, carry):
            for part in range(2):
                for a in range(local_a):
                    tile = recv[slot, p, part, :, a * LANES : (a + 1) * LANES].astype(F32)
                    start = pl.multiple_of((part * outer + p * local_a + a) * STEP, STEP)
                    unpacked[pl.ds(start, STEP), :] = tile
            return carry

        lax.fori_loop(0, groups, body, 0)

    def forward(ch, g):
        rows = [unpacked[pl.ds(j, 2 * outer, stride=STEP), :] for j in range(STEP)]
        wide = jnp.concatenate([row.astype(BF16) for row in rows], axis=1)
        half = jnp.dot(first_t[...], wide, preferred_element_type=F32)
        tc, ts = twiddle[0], twiddle[1]
        turned = []
        for j in range(STEP):
            re = half[:outer, j * LANES : (j + 1) * LANES]
            im = half[outer:, j * LANES : (j + 1) * LANES]
            turned.append(
                jnp.concatenate(
                    [(re * tc + im * ts).astype(BF16), (im * tc - re * ts).astype(BF16)], axis=1
                )
            )
        done = jnp.dot(
            jnp.concatenate(turned, axis=0), fwd_t[...], preferred_element_type=F32
        ).astype(BF16)
        for j in range(STEP):
            r = g * STEP + j
            spec[ch, 0, r] = done[j * outer : (j + 1) * outer, :LANES]
            spec[ch, 1, r] = done[j * outer : (j + 1) * outer, LANES:]

    def inverse(ch, blk, g):
        amount = shifts[blk]
        turned = []
        for j in range(STEP):
            r = g * STEP + j
            re, im = spec[ch, 0, r], spec[ch, 1, r]
            for s in range(1, SMAX + 1):
                hit = amount == s
                re = jnp.where(hit, spec[ch, 0, r + s], re)
                im = jnp.where(hit, spec[ch, 1, r + s], im)
            re, im = re.astype(F32), im.astype(F32)
            c, s_ = cosine[r], sine[r]
            turned.append(
                jnp.concatenate(
                    [(re * c - im * s_).astype(BF16), (re * s_ + im * c).astype(BF16)], axis=1
                )
            )
        mid = jnp.dot(jnp.concatenate(turned, axis=0), inv_t[...], preferred_element_type=F32)
        tc, ts = twiddle[2], twiddle[3]
        columns = []
        for j in range(STEP):
            re = mid[j * outer : (j + 1) * outer, :LANES]
            im = mid[j * outer : (j + 1) * outer, LANES:]
            columns.append(
                jnp.concatenate(
                    [(re * tc - im * ts).astype(BF16), (im * tc + re * ts).astype(BF16)], axis=0
                )
            )
        done = jnp.dot(
            last_t[...], jnp.concatenate(columns, axis=1), preferred_element_type=F32
        )
        for j in range(STEP):
            for part in range(2):
                full = done[part * outer : (part + 1) * outer, j * LANES : (j + 1) * LANES]
                r = g * STEP + j
                zero = jnp.zeros((1, LANES), F32)
                rounded = full.astype(BF16)
                exact = rounded.astype(F32)
                pieces = []
                for h in range(pols):
                    low, high = h * half_rows, (h + 1) * half_rows
                    before = exact[low - 1 : low] if h > 0 else zero
                    after = exact[high : high + 1] if h < pols - 1 else zero
                    pieces.append((exact[low:high], before, after))
                for k in range(pols):
                    main, before, after = pieces[k]
                    for p in range(1, pols):
                        mine = pol_i == p
                        other = pieces[(p + k) % pols]
                        main = jnp.where(mine, other[0], main)
                        before = jnp.where(mine, other[1], before)
                        after = jnp.where(mine, other[2], after)
                    if k == 0:
                        chan = pol_i * chans + ch
                        quad[chan, part, HALF + r] = main.astype(BF16)
                        quad_edge[chan, part, HALF + r, 0:1] = before
                        quad_edge[chan, part, HALF + r, 1:2] = after
                    else:
                        image[ch, k - 1, part, r] = main.astype(BF16)
                        edge[ch, k - 1, part, r, 0:1] = before
                        edge[ch, k - 1, part, r, 1:2] = after

    def loop(count, start, fun):
        def body(i, carry):
            fun(start + i)
            return carry

        lax.fori_loop(0, count, body, 0)

    def relays(array, sems, recvs, ch, side):
        @pl.when(sides[side][1])
        def _():
            for o in range(pols):
                relay(array, sems, recvs, o * chans + ch, side).start()

    def pauli(source, target, r):
        v = [[source[c, part, r].astype(F32) for part in range(2)] for c in range(4)]
        k1 = [(v[0][i] + v[3][i]) * ROOT_HALF for i in range(2)]
        k2 = [(v[0][i] - v[3][i]) * ROOT_HALF for i in range(2)]
        k3 = [(v[1][i] + v[2][i]) * ROOT_HALF for i in range(2)]
        terms = [k[0] * k[0] + k[1] * k[1] for k in (k1, k2, k3)]
        for a, b in ((k1, k2), (k1, k3), (k2, k3)):
            terms.append(a[0] * b[0] + a[1] * b[1])
            terms.append(a[1] * b[0] - a[0] * b[1])
        for i, term in enumerate(terms):
            target[i, r] = term

    def cell_row(r):
        pauli(quad, cells, r)
        pauli(quad_edge, cells_edge, r)

    def pass_on(ch, side):
        landed(ch, rims[side])
        relays(quad, r_send, r_recv, ch, side)
        relays(quad_edge, f_send, f_recv, ch, side)

    def produce(ch, blk):
        inverse(ch, blk * STEP // RBLK, blk)
        for k in range(1, pols):
            e_copy(ch, blk, k).start()
            x_copy(ch, blk, k).start()

    def take_halo(ch, part):
        @pl.when((me < groups - 1) & (me != mid - 1))
        def _():
            halo_copy(ch, part).wait_recv()

        @pl.when(me == mid - 1)
        def _():
            slot = units + ch * halos + part
            z_landed(slot)
            unpack(slot)
            forward(ch, quads + part)

    rims = (0, quads - 1)
    late = list(range(quads - halos, quads))
    for ch in range(chans):
        for part in range(quads):
            unit = ch * quads + part
            z_landed(unit)
            send_step(unit + AHEAD + mylag)
            unpack(unit)
            forward(ch, part)
            if part < halos:

                @pl.when((me > 0) & (me != mid))
                def _(ch=ch, part=part):
                    halo_copy(ch, part).start()

            if part >= halos:
                produce(ch, part - halos)
            if ch > 0:
                if part < halos:
                    take_halo(ch - 1, part)
                    produce(ch - 1, late[part])
                if part == halos - 1:
                    pass_on(ch - 1, 0)
                if part == quads - 2:
                    pass_on(ch - 1, 1)
                    x_sent(ch - 1)
            if unit >= DRAIN:
                z_sent(unit - DRAIN)

    last = chans - 1
    for part in range(halos):
        take_halo(last, part)
    for blk in late[::-1]:
        produce(last, blk)
    for ch in range(chans):
        if ch < last:
            for blk in range(1, quads - 1):
                landed(ch, blk)

        @pl.when((me > 0) & (me != mid))
        def _(ch=ch):
            for part in range(halos):
                halo_copy(ch, part).wait_send()

    for unit in range(max(0, units - DRAIN), units):
        z_sent(unit)

    @pl.when(me != mid - 1)
    def _():
        for slot in range(units, units + chans * halos):
            if mid > 0:
                some = recv.at[slot, 0]
                pltpu.make_async_copy(some, some, z_send.at[slot]).wait()

    for side in range(2):
        pass_on(last, side)
        loop(STEP, HALF + rims[side] * STEP, cell_row)
    for blk in range(1, quads - 1):
        landed(last, blk)
        loop(STEP, HALF + blk * STEP, cell_row)
    x_sent(last)
    for array, sems, recvs in ((quad, r_send, r_recv), (quad_edge, f_send, f_recv)):
        relayed(array, sems)
        rows = array.at[:, :, pl.ds(0, HALF)]
        for side, cond in ((0, me < groups - 1), (1, me > 0)):

            @pl.when(cond)
            def _(side=side, rows=rows, recvs=recvs):
                pltpu.make_async_copy(rows, rows, recvs.at[side]).wait()

    loop(HALF, 0, cell_row)
    loop(HALF, bins + HALF, cell_row)

    def range_sum(x):
        two = x[:-1] + x[1:]
        four = two[:-2] + two[2:]
        return four[:bins] + two[4 : 4 + bins] + x[6 : 6 + bins]

    lane = lax.broadcasted_iota(jnp.int32, (bins, half_rows, LANES), 2)

    def component(i):
        slot = i % SLOTS
        for j in range(half_rows // 8):
            padded[slot, :, 8 + j * 8 : 16 + j * 8, :] = range_sum(cells[i, :, j * 8 : (j + 1) * 8, :])
        rim = range_sum(cells_edge[i])
        padded[slot, :, 7:8, :] = rim[:, 0:1, :]
        padded[slot, :, 8 + half_rows : 9 + half_rows, :] = rim[:, 1:2, :]
        mid = padded[slot, :, 8 : 8 + half_rows, :]
        side = jnp.where(
            lane < LANES // 2,
            padded[slot, :, 9 : 9 + half_rows, :],
            padded[slot, :, 7 : 7 + half_rows, :],
        )
        flat = (bins * half_rows, LANES)
        both = jnp.concatenate(
            [mid.reshape(flat).astype(BF16), side.reshape(flat).astype(BF16)], axis=1
        )
        total = jnp.dot(both, band[...], preferred_element_type=F32)
        result[slot] = total * (1.0 / (WIN * WIN))
        for a in range(half_rows):
            piece = result[slot, pl.ds(a, bins, stride=half_rows), :]
            out[i, :, a * LANES : (a + 1) * LANES] = piece.astype(BF16)

    for i in range(9):
        component(i)


def shards(echoes, migration, fm_rate):
    rng_size = lax.axis_size("rng")
    groups = lax.axis_size("pulse") * rng_size
    pols = lax.axis_size("pol")
    chans = echoes.shape[0]
    pulses = echoes.shape[3]
    bins = echoes.shape[2] // groups
    outer = groups * pulses // LANES
    half_rows = outer // pols
    units = chans * (bins // STEP)
    consts = tables(outer)
    vmem = pl.BlockSpec(memory_space=pltpu.VMEM)
    anywhere = pl.BlockSpec(memory_space=pltpu.HBM)
    dma = pltpu.SemaphoreType.DMA
    tall = bins + 2 * HALF
    return pl.pallas_call(
        functools.partial(kernel, chans, groups, pols, bins, outer, rng_size),
        out_shape=pltpu.VMEM((9, bins, half_rows * LANES), BF16),
        in_specs=[
            anywhere,
            anywhere,
            pl.BlockSpec(memory_space=pltpu.SMEM),
        ]
        + [anywhere] * len(consts),
        out_specs=vmem,
        scratch_shapes=[
            pltpu.VMEM(migration.shape, jnp.int32),
            *(pltpu.VMEM(table.shape, table.dtype) for table in consts),
            dma((1 + len(consts),)),
            pltpu.VMEM((units + chans * (SMAX // STEP), groups, 2, STEP, pulses), BF16),
            pltpu.VMEM((2 * outer * STEP, LANES), F32),
            pltpu.VMEM((chans, 2, bins + SMAX, outer, LANES), BF16),
            pltpu.VMEM((chans, pols - 1, 2, bins, half_rows, LANES), BF16),
            pltpu.VMEM((chans, pols - 1, 2, bins, 2, LANES), F32),
            pltpu.VMEM((4, 2, tall, half_rows, LANES), BF16),
            pltpu.VMEM((4, 2, tall, 2, LANES), F32),
            pltpu.VMEM((migration.shape[0], outer, LANES), BF16),
            pltpu.VMEM((outer, LANES), F32),
            pltpu.VMEM((bins, outer, LANES), F32),
            pltpu.VMEM((bins, outer, LANES), F32),
            pltpu.VMEM((9, tall, half_rows, LANES), F32),
            pltpu.VMEM((9, tall, 2, LANES), F32),
            pltpu.VMEM((SLOTS, bins, half_rows + 16, LANES), F32),
            pltpu.VMEM((SLOTS, bins * half_rows, LANES), F32),
            dma((units + chans * (SMAX // STEP),)),
            dma((units + chans * (SMAX // STEP),)),
            dma((chans, SMAX // STEP)),
            dma((chans, SMAX // STEP)),
            dma((chans,)),
            dma((chans, bins // STEP)),
            dma((chans,)),
            dma((chans, bins // STEP)),
            dma((2,)),
            dma((2,)),
            dma((2,)),
            dma((2,)),
        ],
        compiler_params=pltpu.CompilerParams(
            collective_id=0, has_side_effects=True, vmem_limit_bytes=58 * 1024 * 1024
        ),
    )(echoes, migration, fm_rate, *consts)


def solution(mesh):
    placed = (
        P(("scene", "pol"), None, None, ("pulse", "rng")),
        P(("scene", "pulse", "rng"), None),
        P(("scene", "pulse", "rng")),
    )
    return jax.shard_map(
        shards,
        mesh=mesh,
        in_specs=placed,
        out_specs=P(None, ("scene", "pulse", "rng"), "pol"),
        check_vma=False,
    )
```

```python
import functools
import math

import jax
import jax.numpy as jnp
import numpy as np
from jax import lax
from jax.experimental import pallas as pl
from jax.experimental.pallas import tpu as pltpu
from jax.sharding import PartitionSpec as P

RBLK = 8
SMAX = 8
WIN = 7
HALF = WIN // 2
LANES = 128
STEP = 4
SLOTS = 3
AHEAD = 3
LAG = 2
FIRST = 0
RAW = 5
REVERSE = False
ROOT_HALF = 0.7071067811865476
MESH = pl.DeviceIdType.MESH
F32 = jnp.float32
BF16 = jnp.bfloat16


def fit(function, degree):
    nodes = (np.cos(np.pi * (np.arange(64) + 0.5) / 64) + 1) / 8
    poly = np.polynomial.Chebyshev.fit(nodes, function(nodes), degree, domain=[0, 0.25])
    return [float(v) for v in poly.convert(kind=np.polynomial.Polynomial).coef]


SIN_COEF = fit(lambda y: np.sin(2 * np.pi * np.sqrt(y)) / np.sqrt(y), 7)
COS_COEF = fit(lambda y: np.cos(2 * np.pi * np.sqrt(y)), 7)


def horner(coefs, y):
    total = jnp.full_like(y, coefs[-1])
    for coef in coefs[-2::-1]:
        total = total * y + coef
    return total


def trig(period, height, width):
    index = np.arange(height)[:, None] * np.arange(width)[None, :] % period
    return np.cos(2 * np.pi * index / period), np.sin(2 * np.pi * index / period)


def tables(outer):
    size = outer * LANES
    oc, os_ = trig(outer, outer, outer)
    scale = 1.0 / math.sqrt(outer)
    first = np.block([[oc, os_], [-os_, oc]]) * scale
    last = np.block([[oc, -os_], [os_, oc]]) * scale
    ic, is_ = trig(LANES, LANES, LANES)
    fwd = np.block([[ic, -is_], [is_, ic]])
    inv = np.block([[ic, is_], [-is_, ic]])
    tc, ts = trig(size, outer, LANES)
    row = np.arange(LANES)
    gap = row[:, None] - row[None, :]
    near = np.abs(gap) <= HALF
    wrap = np.abs(np.abs(gap) - LANES) <= HALF
    band = np.concatenate([near, wrap], axis=0)
    per_row = LANES // outer
    spread = np.zeros((per_row * outer, LANES))
    for u in range(outer):
        for h in range(per_row):
            spread[h * outer + u, per_row * u + h] = 1
    short = lambda v: np.asarray(v, np.float32).astype(BF16).astype(np.float32)

    def gain(v):
        return float(np.sum(v * short(v)) / np.sum(v * v))

    root = math.sqrt(LANES)
    there, back = root * gain(first) * gain(fwd), root * gain(inv) * gain(last)
    twiddle = np.stack([tc / there, ts / there, tc / back, ts / back])
    fill = lambda v, width: np.pad(v, ((0, 0), (0, width - v.shape[1])))
    slim = np.concatenate([fill(first, LANES), fill(last, LANES), spread])
    wide = np.concatenate([fwd, inv, fill(band, 2 * LANES)])
    return jnp.asarray(wide, BF16), jnp.asarray(slim, BF16), jnp.asarray(twiddle, F32)


def kernel(
    chans, groups, pols, bins, outer, rng_size,
    echo, mig_hbm, rate, wide_hbm, slim_hbm, twiddle_hbm,
    out,
    mig, wide_t, slim_t, twiddle, t_sem,
    recv, unpacked, spec, image, edge, quad, quad_edge, shifts, mig_rows, cosine, sine,
    cells, cells_edge, padded, result,
    z_send, z_recv, h_send, h_recv, x_send, x_recv, e_send, e_recv, r_send, r_recv, f_send, f_recv,
):
    half_rows = outer // pols
    local_a = outer // groups
    pulse_i, rng_i, pol_i = (lax.axis_index(n) for n in ("pulse", "rng", "pol"))
    me = pulse_i * rng_size + rng_i

    def member(q):
        return {"pulse": q // rng_size, "rng": lax.rem(q, rng_size)}

    fetches = [
        pltpu.make_async_copy(source, target, t_sem.at[i])
        for i, (source, target) in enumerate(
            ((mig_hbm, mig), (slim_hbm, slim_t), (twiddle_hbm, twiddle), (wide_hbm, wide_t))
        )
    ]
    for fetch in fetches:
        fetch.start()
    two = 2 * outer
    first_t, last_t = slim_t.at[0:two, 0:two], slim_t.at[two : 2 * two, 0:two]
    fwd_t, inv_t = wide_t.at[0 : 2 * LANES], wide_t.at[2 * LANES : 4 * LANES]
    band = wide_t.at[4 * LANES : 6 * LANES, 0:LANES]

    barrier = pltpu.get_barrier_semaphore()

    def greet_group(k, carry):
        pl.semaphore_signal(
            barrier, inc=1, device_id=member(lax.rem(me + k, groups)), device_id_type=MESH
        )
        return carry

    lax.fori_loop(1, groups, greet_group, 0)
    for k in range(1, pols):
        pl.semaphore_signal(
            barrier, inc=1, device_id={"pol": lax.rem(pol_i + k, pols)}, device_id_type=MESH
        )
    pl.semaphore_wait(barrier, groups - 1 + pols - 1)

    depth = groups // rng_size
    quads = bins // STEP
    halos = SMAX // STEP
    units = chans * quads
    mid = rng_size * (depth // 2)

    def z_copy(unit, first, slot, q):
        ch, part = unit // quads, lax.rem(unit, quads)
        start = pl.multiple_of(first * bins + part * STEP, STEP)
        return pltpu.make_async_remote_copy(
            src_ref=echo.at[ch, :, pl.ds(start, STEP), :],
            dst_ref=recv.at[slot, me],
            send_sem=z_send.at[slot // units],
            recv_sem=z_recv.at[slot],
            device_id=member(q),
            device_id_type=MESH,
        )

    def own_copy(unit, first, slot):
        ch, part = unit // quads, lax.rem(unit, quads)
        start = pl.multiple_of(first * bins + part * STEP, STEP)
        return pltpu.make_async_copy(
            echo.at[ch, :, pl.ds(start, STEP), :], recv.at[slot, me], z_recv.at[slot]
        )

    def z_landed(slot):
        pltpu.make_async_copy(recv.at[slot], recv.at[slot], z_recv.at[slot]).wait()

    def place(core):
        return rng_size - 1 - core if REVERSE else core

    def send_step(step):
        def to_layer(layer, near):
            for j in range(rng_size):
                q = layer * rng_size + j
                unit = step - LAG * place(j) - FIRST * jnp.minimum(layer, 1)
                valid = (unit >= 0) & (unit < units)
                if near:

                    @pl.when(valid & (rng_i == j))
                    def _():
                        own_copy(unit, me, unit).start()

                    valid = valid & (rng_i != j)

                @pl.when(valid)
                def _():
                    z_copy(unit, q, unit, q).start()

        def send_echo(i, carry):
            gap = depth - 1 - i
            for sign in (1, -1):
                layer = pulse_i + sign * gap

                @pl.when((layer >= 0) & (layer < depth))
                def _(layer=layer):
                    to_layer(layer, False)

            return carry

        lax.fori_loop(0, depth - 1, send_echo, 0)
        to_layer(pulse_i, True)
        early = step - FIRST - RAW
        slot = units + early // quads * halos + lax.rem(early, quads)
        valid = (early >= 0) & (early < units) & (lax.rem(early, quads) < halos)
        if mid > 0:

            @pl.when(valid & (me == mid - 1))
            def _():
                own_copy(early, mid, slot).start()

            @pl.when(valid & (me != mid - 1))
            def _():
                z_copy(early, mid, slot, mid - 1).start()

    mylag = LAG * place(rng_i) + FIRST * jnp.minimum(pulse_i, 1)

    def opening(step, carry):
        send_step(step)
        return carry

    lax.fori_loop(0, AHEAD + mylag, opening, 0)

    def zero_edges():
        @pl.when(me == groups - 1)
        def _():
            spec[:, :, bins:, :, :] = jnp.zeros((chans, 2, SMAX, outer, LANES), BF16)
            quad[:, :, HALF + bins :, :, :] = jnp.zeros((4, 2, HALF, half_rows, LANES), BF16)
            quad_edge[:, :, HALF + bins :, :, :] = jnp.zeros((4, 2, HALF, 2, LANES), F32)

        @pl.when(me == 0)
        def _():
            quad[:, :, :HALF, :, :] = jnp.zeros((4, 2, HALF, half_rows, LANES), BF16)
            quad_edge[:, :, :HALF, :, :] = jnp.zeros((4, 2, HALF, 2, LANES), F32)

    zero_edges()
    for fetch in fetches:
        fetch.wait()

    per_row = LANES // outer
    for k in range(mig.shape[0]):
        for u in range(outer):
            mig_rows[u : u + 1, :] = mig[k : k + 1, u * LANES : (u + 1) * LANES].astype(F32)
        turned = mig_rows[...].T.astype(BF16)
        total = jnp.zeros((outer, LANES), F32)
        for h in range(per_row):
            total = total + jnp.dot(
                turned[h * outer : (h + 1) * outer],
                slim_t[(2 * two + h * outer) : (2 * two + (h + 1) * outer)],
                preferred_element_type=F32,
            )
        shifts[k] = total.astype(BF16)

    size = outer * LANES
    position = lax.broadcasted_iota(jnp.int32, (outer, LANES), 0) + outer * (
        lax.broadcasted_iota(jnp.int32, (outer, LANES), 1)
    )
    centred = jnp.where(position < size // 2, position, position - size).astype(F32)
    quadratic = centred * centred / size

    def phase_row(r, carry):
        turns = (0.5 * rate[r]) * quadratic
        turns = turns - jnp.round(turns)
        square = turns * turns
        cosine[r] = horner(COS_COEF, square)
        sine[r] = horner(SIN_COEF, square) * turns
        return carry

    lax.fori_loop(0, bins, phase_row, 0)

    def halo_copy(ch, part):
        return pltpu.make_async_remote_copy(
            src_ref=spec.at[ch, :, pl.ds(part * STEP, STEP)],
            dst_ref=spec.at[ch, :, pl.ds(bins + part * STEP, STEP)],
            send_sem=h_send,
            recv_sem=h_recv.at[ch, part],
            device_id=member(jnp.maximum(me - 1, 0)),
            device_id_type=MESH,
        )

    def x_copy(ch, blk, k):
        return pltpu.make_async_remote_copy(
            src_ref=image.at[ch, k - 1, :, pl.ds(blk * STEP, STEP)],
            dst_ref=quad.at[pol_i * chans + ch, :, pl.ds(HALF + blk * STEP, STEP)],
            send_sem=x_send,
            recv_sem=x_recv.at[ch, blk],
            device_id={"pol": lax.rem(pol_i + k, pols)},
            device_id_type=MESH,
        )

    def e_copy(ch, blk, k):
        return pltpu.make_async_remote_copy(
            src_ref=edge.at[ch, k - 1, :, pl.ds(blk * STEP, STEP)],
            dst_ref=quad_edge.at[pol_i * chans + ch, :, pl.ds(HALF + blk * STEP, STEP)],
            send_sem=e_send,
            recv_sem=e_recv.at[ch, blk],
            device_id={"pol": lax.rem(pol_i + k, pols)},
            device_id_type=MESH,
        )

    def landed(ch, blk):
        if pols > 1:
            rows = pl.ds(HALF + blk * STEP, STEP)
            some = quad.at[pl.ds(0, pols - 1), :, rows]
            few = quad_edge.at[pl.ds(0, pols - 1), :, rows]
            pltpu.make_async_copy(some, some, x_recv.at[ch, blk]).wait()
            pltpu.make_async_copy(few, few, e_recv.at[ch, blk]).wait()

    def relay(array, sems, recvs, chan, side):
        take = HALF if side == 0 else bins
        put = HALF + bins if side == 0 else 0
        target = jnp.maximum(me - 1, 0) if side == 0 else jnp.minimum(me + 1, groups - 1)
        return pltpu.make_async_remote_copy(
            src_ref=array.at[chan, :, pl.ds(take, HALF)],
            dst_ref=array.at[chan, :, pl.ds(put, HALF)],
            send_sem=sems.at[side],
            recv_sem=recvs.at[side],
            device_id=member(target),
            device_id_type=MESH,
        )

    sides = ((0, me > 0), (1, me < groups - 1))

    def relayed(array, sems):
        rows = array.at[:, :, pl.ds(0, HALF)]
        for side, cond in sides:

            @pl.when(cond)
            def _(side=side):
                pltpu.make_async_copy(rows, rows, sems.at[side]).wait()

    def unpack(slot):
        def body(p, carry):
            for part in range(2):
                for a in range(local_a):
                    tile = recv[slot, p, part, :, a * LANES : (a + 1) * LANES].astype(F32)
                    start = pl.multiple_of((part * outer + p * local_a + a) * STEP, STEP)
                    unpacked[pl.ds(start, STEP), :] = tile
            return carry

        lax.fori_loop(0, groups, body, 0)

    def forward(ch, g):
        rows = [unpacked[pl.ds(j, 2 * outer, stride=STEP), :] for j in range(STEP)]
        wide = jnp.concatenate([row.astype(BF16) for row in rows], axis=1)
        half = jnp.dot(first_t[...], wide, preferred_element_type=F32)
        tc, ts = twiddle[0], twiddle[1]
        turned = []
        for j in range(STEP):
            re = half[:outer, j * LANES : (j + 1) * LANES]
            im = half[outer:, j * LANES : (j + 1) * LANES]
            turned.append(
                jnp.concatenate(
                    [(re * tc + im * ts).astype(BF16), (im * tc - re * ts).astype(BF16)], axis=1
                )
            )
        done = jnp.dot(
            jnp.concatenate(turned, axis=0), fwd_t[...], preferred_element_type=F32
        ).astype(BF16)
        for j in range(STEP):
            r = g * STEP + j
            spec[ch, 0, r] = done[j * outer : (j + 1) * outer, :LANES]
            spec[ch, 1, r] = done[j * outer : (j + 1) * outer, LANES:]

    def inverse(ch, blk, g):
        amount = shifts[blk]
        turned = []
        for j in range(STEP):
            r = g * STEP + j
            re, im = spec[ch, 0, r], spec[ch, 1, r]
            for s in range(1, SMAX + 1):
                hit = amount == s
                re = jnp.where(hit, spec[ch, 0, r + s], re)
                im = jnp.where(hit, spec[ch, 1, r + s], im)
            re, im = re.astype(F32), im.astype(F32)
            c, s_ = cosine[r], sine[r]
            turned.append(
                jnp.concatenate(
                    [(re * c - im * s_).astype(BF16), (re * s_ + im * c).astype(BF16)], axis=1
                )
            )
        mid = jnp.dot(jnp.concatenate(turned, axis=0), inv_t[...], preferred_element_type=F32)
        tc, ts = twiddle[2], twiddle[3]
        columns = []
        for j in range(STEP):
            re = mid[j * outer : (j + 1) * outer, :LANES]
            im = mid[j * outer : (j + 1) * outer, LANES:]
            columns.append(
                jnp.concatenate(
                    [(re * tc - im * ts).astype(BF16), (im * tc + re * ts).astype(BF16)], axis=0
                )
            )
        done = jnp.dot(
            last_t[...], jnp.concatenate(columns, axis=1), preferred_element_type=F32
        )
        for j in range(STEP):
            for part in range(2):
                full = done[part * outer : (part + 1) * outer, j * LANES : (j + 1) * LANES]
                r = g * STEP + j
                zero = jnp.zeros((1, LANES), F32)
                rounded = full.astype(BF16)
                exact = rounded.astype(F32)
                pieces = []
                for h in range(pols):
                    low, high = h * half_rows, (h + 1) * half_rows
                    before = exact[low - 1 : low] if h > 0 else zero
                    after = exact[high : high + 1] if h < pols - 1 else zero
                    pieces.append((exact[low:high], before, after))
                for k in range(pols):
                    main, before, after = pieces[k]
                    for p in range(1, pols):
                        mine = pol_i == p
                        other = pieces[(p + k) % pols]
                        main = jnp.where(mine, other[0], main)
                        before = jnp.where(mine, other[1], before)
                        after = jnp.where(mine, other[2], after)
                    if k == 0:
                        chan = pol_i * chans + ch
                        quad[chan, part, HALF + r] = main.astype(BF16)
                        quad_edge[chan, part, HALF + r, 0:1] = before
                        quad_edge[chan, part, HALF + r, 1:2] = after
                    else:
                        image[ch, k - 1, part, r] = main.astype(BF16)
                        edge[ch, k - 1, part, r, 0:1] = before
                        edge[ch, k - 1, part, r, 1:2] = after

    def loop(count, start, fun):
        def body(i, carry):
            fun(start + i)
            return carry

        lax.fori_loop(0, count, body, 0)

    def pauli(source, target, r):
        v = [[source[c, part, r].astype(F32) for part in range(2)] for c in range(4)]
        k1 = [(v[0][i] + v[3][i]) * ROOT_HALF for i in range(2)]
        k2 = [(v[0][i] - v[3][i]) * ROOT_HALF for i in range(2)]
        k3 = [(v[1][i] + v[2][i]) * ROOT_HALF for i in range(2)]
        terms = [k[0] * k[0] + k[1] * k[1] for k in (k1, k2, k3)]
        for a, b in ((k1, k2), (k1, k3), (k2, k3)):
            terms.append(a[0] * b[0] + a[1] * b[1])
            terms.append(a[1] * b[0] - a[0] * b[1])
        for i, term in enumerate(terms):
            target[i, r] = term

    def cell_row(r):
        pauli(quad, cells, r)
        pauli(quad_edge, cells_edge, r)

    def rim_copies(ch, side, owner):
        @pl.when(sides[side][1])
        def _():
            relay(quad, r_send, r_recv, owner * chans + ch, side).start()
            relay(quad_edge, f_send, f_recv, owner * chans + ch, side).start()

    def pass_on(ch, side):
        landed(ch, rims[side])
        for k in range(side, pols):
            rim_copies(ch, side, lax.rem(pol_i + k, pols))

    def produce(ch, blk):
        inverse(ch, blk * STEP // RBLK, blk)
        for k in range(1, pols):
            e_copy(ch, blk, k).start()
            x_copy(ch, blk, k).start()

        @pl.when(blk == quads - 1)
        def _():
            rim_copies(ch, 1, pol_i)

    def take_halo(ch, part):
        @pl.when((me < groups - 1) & (me != mid - 1))
        def _():
            halo_copy(ch, part).wait_recv()

        @pl.when(me == mid - 1)
        def _():
            slot = units + ch * halos + part
            z_landed(slot)
            unpack(slot)
            forward(ch, quads + part)

    rims = (0, quads - 1)
    late = list(range(quads - halos, quads))
    for ch in range(chans):
        for part in range(quads):
            unit = ch * quads + part
            z_landed(unit)
            send_step(unit + AHEAD + mylag)
            unpack(unit)
            forward(ch, part)
            if part < halos:

                @pl.when((me > 0) & (me != mid))
                def _(ch=ch, part=part):
                    halo_copy(ch, part).start()

            if part >= halos and (part < quads - 1 or ch < chans - 1):
                produce(ch, part - halos)
            if ch > 0:
                if part < halos:
                    take_halo(ch - 1, part)
                    produce(ch - 1, late[part])

    def range_sum(x, count):
        two = x[:-1] + x[1:]
        four = two[:-2] + two[2:]
        return four[:count] + two[4 : 4 + count] + x[6 : 6 + count]

    def component(i, low, high):
        slot, count = i % SLOTS, high - low
        tall = slice(low, high + 2 * HALF)
        for j in range(half_rows // 8):
            padded[slot, :count, 8 + j * 8 : 16 + j * 8, :] = range_sum(
                cells[i, tall, j * 8 : (j + 1) * 8, :], count
            )
        rim = range_sum(cells_edge[i, tall], count)
        padded[slot, :count, 7:8, :] = rim[:, 0:1, :]
        padded[slot, :count, 8 + half_rows : 9 + half_rows, :] = rim[:, 1:2, :]
        center = padded[slot, :count, 8 : 8 + half_rows, :]
        lane = lax.broadcasted_iota(jnp.int32, (count, half_rows, LANES), 2)
        side = jnp.where(
            lane < LANES // 2,
            padded[slot, :count, 9 : 9 + half_rows, :],
            padded[slot, :count, 7 : 7 + half_rows, :],
        )
        flat = (count * half_rows, LANES)
        both = jnp.concatenate(
            [center.reshape(flat).astype(BF16), side.reshape(flat).astype(BF16)], axis=1
        )
        total = jnp.dot(both, band[...], preferred_element_type=F32)
        total = total * (1.0 / (WIN * WIN))
        for r in range(count):
            start = (low + r) * (half_rows + 8)
            result[i, start : start + half_rows] = total[r * half_rows : (r + 1) * half_rows]

    def window(low, high):
        for i in range(9):
            component(i, low, high)

    def take_rim(side):
        @pl.when((me < groups - 1) if side == 0 else (me > 0))
        def _():
            for array, recvs in ((quad, r_recv), (quad_edge, f_recv)):
                rows = array.at[:, :, pl.ds(0, HALF)]
                pltpu.make_async_copy(rows, rows, recvs.at[side]).wait()

        loop(HALF, bins + HALF if side == 0 else 0, cell_row)

    def take_quad(blk):
        landed(last, blk)
        loop(STEP, HALF + blk * STEP, cell_row)

    last = chans - 1
    lagging = place(rng_i) == rng_size - 1
    leading = place(rng_i) != rng_size - 1
    inner = quads - 1 - halos

    def take_halos():
        for part in range(halos):
            take_halo(last, part)

    pl.when(lagging)(take_halos)
    produce(last, jnp.where(lagging, quads - 1, inner))
    pl.when(leading)(take_halos)
    produce(last, jnp.where(lagging, inner, quads - 1))
    for blk in late[:-1]:
        produce(last, blk)
    for ch in range(chans):
        if ch < last:
            for side in range(2):
                pass_on(ch, side)
            for blk in range(1, quads - 1):
                landed(ch, blk)
    pass_on(last, 0)
    loop(STEP, HALF, cell_row)
    early = (quads - halos) * STEP - HALF

    def take_rim_quad():
        pass_on(last, 1)
        loop(STEP, HALF + (quads - 1) * STEP, cell_row)

    @pl.when(lagging)
    def _():
        take_rim_quad()
        for blk in range(1, quads - halos):
            take_quad(blk)
        take_rim(1)
        window(0, early)
        for blk in range(quads - halos, quads - 1):
            take_quad(blk)
        take_rim(0)
        window(early, bins)

    @pl.when(leading)
    def _():
        for blk in range(1, quads - halos):
            take_quad(blk)
        take_rim_quad()
        for blk in range(quads - halos, quads - 1):
            take_quad(blk)
        window(HALF, bins - HALF)
        take_rim(0)
        window(bins - HALF, bins)
        take_rim(1)
        window(0, HALF)

    for i in range(9):
        for a in range(half_rows):
            piece = result[i, pl.ds(a, bins, stride=half_rows + 8), :]
            out[i, :, a * LANES : (a + 1) * LANES] = piece.astype(BF16)

    def drain(array, sem):
        pltpu.make_async_copy(array, array, sem).wait()

    drain(recv.at[pl.ds(0, units), pl.ds(0, groups - 1)], z_send.at[0])

    @pl.when(me != mid - 1)
    def _():
        drain(recv.at[pl.ds(0, chans * halos), 0], z_send.at[1])

    @pl.when((me > 0) & (me != mid))
    def _():
        drain(spec.at[:, :, pl.ds(0, SMAX)], h_send)

    if pols > 1:
        drain(image, x_send)
        drain(edge, e_send)
    relayed(quad, r_send)
    relayed(quad_edge, f_send)


def shards(echoes, migration, fm_rate):
    rng_size = lax.axis_size("rng")
    groups = lax.axis_size("pulse") * rng_size
    pols = lax.axis_size("pol")
    chans = echoes.shape[0]
    pulses = echoes.shape[3]
    bins = echoes.shape[2] // groups
    outer = groups * pulses // LANES
    half_rows = outer // pols
    units = chans * (bins // STEP)
    consts = tables(outer)
    vmem = pl.BlockSpec(memory_space=pltpu.VMEM)
    anywhere = pl.BlockSpec(memory_space=pltpu.HBM)
    dma = pltpu.SemaphoreType.DMA
    tall = bins + 2 * HALF
    return pl.pallas_call(
        functools.partial(kernel, chans, groups, pols, bins, outer, rng_size),
        out_shape=pltpu.VMEM((9, bins, half_rows * LANES), BF16),
        in_specs=[
            anywhere,
            anywhere,
            pl.BlockSpec(memory_space=pltpu.SMEM),
        ]
        + [anywhere] * len(consts),
        out_specs=vmem,
        scratch_shapes=[
            pltpu.VMEM(migration.shape, jnp.int32),
            *(pltpu.VMEM(table.shape, table.dtype) for table in consts),
            dma((1 + len(consts),)),
            pltpu.VMEM((units + chans * (SMAX // STEP), groups, 2, STEP, pulses), BF16),
            pltpu.VMEM((2 * outer * STEP, LANES), F32),
            pltpu.VMEM((chans, 2, bins + SMAX, outer, LANES), BF16),
            pltpu.VMEM((chans, pols - 1, 2, bins, half_rows, LANES), BF16),
            pltpu.VMEM((chans, pols - 1, 2, bins, 2, LANES), F32),
            pltpu.VMEM((4, 2, tall, half_rows, LANES), BF16),
            pltpu.VMEM((4, 2, tall, 2, LANES), F32),
            pltpu.VMEM((migration.shape[0], outer, LANES), BF16),
            pltpu.VMEM((outer, LANES), F32),
            pltpu.VMEM((bins, outer, LANES), F32),
            pltpu.VMEM((bins, outer, LANES), F32),
            pltpu.VMEM((9, tall, half_rows, LANES), F32),
            pltpu.VMEM((9, tall, 2, LANES), F32),
            pltpu.VMEM((SLOTS, bins, half_rows + 16, LANES), F32),
            pltpu.VMEM((9, bins * (half_rows + 8), LANES), F32),
            dma((2,)),
            dma((units + chans * (SMAX // STEP),)),
            dma,
            dma((chans, SMAX // STEP)),
            dma,
            dma((chans, bins // STEP)),
            dma,
            dma((chans, bins // STEP)),
            dma((2,)),
            dma((2,)),
            dma((2,)),
            dma((2,)),
        ],
        compiler_params=pltpu.CompilerParams(
            collective_id=0, has_side_effects=True, vmem_limit_bytes=58 * 1024 * 1024
        ),
    )(echoes, migration, fm_rate, *consts)


def solution(mesh):
    placed = (
        P(("scene", "pol"), None, None, ("pulse", "rng")),
        P(("scene", "pulse", "rng"), None),
        P(("scene", "pulse", "rng")),
    )
    return jax.shard_map(
        shards,
        mesh=mesh,
        in_specs=placed,
        out_specs=P(None, ("scene", "pulse", "rng"), "pol"),
        check_vma=False,
    )
```

```python
import functools
import math

import jax
import jax.numpy as jnp
import numpy as np
from jax import lax
from jax.experimental import pallas as pl
from jax.experimental.pallas import tpu as pltpu
from jax.sharding import PartitionSpec as P

RBLK = 8
SMAX = 8
WIN = 7
HALF = WIN // 2
LANES = 128
STEP = 4
SLOTS = 3
AHEAD = 3
LAG = 2
FIRST = 0
RAW = 5
REVERSE = False
ROOT_HALF = 0.7071067811865476
MESH = pl.DeviceIdType.MESH
F32 = jnp.float32
BF16 = jnp.bfloat16


def fit(function, degree):
    nodes = (np.cos(np.pi * (np.arange(64) + 0.5) / 64) + 1) / 8
    poly = np.polynomial.Chebyshev.fit(nodes, function(nodes), degree, domain=[0, 0.25])
    return [float(v) for v in poly.convert(kind=np.polynomial.Polynomial).coef]


SIN_COEF = fit(lambda y: np.sin(2 * np.pi * np.sqrt(y)) / np.sqrt(y), 7)
COS_COEF = fit(lambda y: np.cos(2 * np.pi * np.sqrt(y)), 7)


def horner(coefs, y):
    total = jnp.full_like(y, coefs[-1])
    for coef in coefs[-2::-1]:
        total = total * y + coef
    return total


def trig(period, height, width):
    index = np.arange(height)[:, None] * np.arange(width)[None, :] % period
    return np.cos(2 * np.pi * index / period), np.sin(2 * np.pi * index / period)


def tables(outer):
    size = outer * LANES
    oc, os_ = trig(outer, outer, outer)
    scale = 1.0 / math.sqrt(outer)
    first = np.block([[oc, os_], [-os_, oc]]) * scale
    last = np.block([[oc, -os_], [os_, oc]]) * scale
    ic, is_ = trig(LANES, LANES, LANES)
    fwd = np.block([[ic, -is_], [is_, ic]])
    inv = np.block([[ic, is_], [-is_, ic]])
    tc, ts = trig(size, outer, LANES)
    row = np.arange(LANES)
    gap = row[:, None] - row[None, :]
    near = np.abs(gap) <= HALF
    wrap = np.abs(np.abs(gap) - LANES) <= HALF
    band = np.concatenate([near, wrap], axis=0)
    per_row = LANES // outer
    spread = np.zeros((per_row * outer, LANES))
    for u in range(outer):
        for h in range(per_row):
            spread[h * outer + u, per_row * u + h] = 1
    short = lambda v: np.asarray(v, np.float32).astype(BF16).astype(np.float32)

    def gain(v):
        return float(np.sum(v * short(v)) / np.sum(v * v))

    root = math.sqrt(LANES)
    there, back = root * gain(first) * gain(fwd), root * gain(inv) * gain(last)
    twiddle = np.stack([tc / there, ts / there, tc / back, ts / back])
    fill = lambda v, width: np.pad(v, ((0, 0), (0, width - v.shape[1])))
    slim = np.concatenate([fill(first, LANES), fill(last, LANES), spread])
    wide = np.concatenate([fwd, inv, fill(band, 2 * LANES)])
    return jnp.asarray(wide, BF16), jnp.asarray(slim, BF16), jnp.asarray(twiddle, F32)


def kernel(
    chans, groups, pols, bins, outer, rng_size,
    echo, mig_hbm, rate, wide_hbm, slim_hbm, twiddle_hbm,
    out,
    mig, wide_t, slim_t, twiddle, t_sem,
    recv, unpacked, spec, image, edge, quad, quad_edge, shifts, mig_rows, cosine, sine,
    cells, cells_edge, padded, result,
    z_send, z_recv, h_send, h_recv, x_send, x_recv, r_send, r_recv,
):
    half_rows = outer // pols
    local_a = outer // groups
    pulse_i, rng_i, pol_i = (lax.axis_index(n) for n in ("pulse", "rng", "pol"))
    me = pulse_i * rng_size + rng_i

    def member(q):
        return {"pulse": q // rng_size, "rng": lax.rem(q, rng_size)}

    fetches = [
        pltpu.make_async_copy(source, target, t_sem.at[i])
        for i, (source, target) in enumerate(
            ((mig_hbm, mig), (slim_hbm, slim_t), (twiddle_hbm, twiddle), (wide_hbm, wide_t))
        )
    ]
    for fetch in fetches:
        fetch.start()
    two = 2 * outer
    first_t, last_t = slim_t.at[0:two, 0:two], slim_t.at[two : 2 * two, 0:two]
    fwd_t, inv_t = wide_t.at[0 : 2 * LANES], wide_t.at[2 * LANES : 4 * LANES]
    band = wide_t.at[4 * LANES : 6 * LANES, 0:LANES]

    barrier = pltpu.get_barrier_semaphore()

    def greet_group(k, carry):
        pl.semaphore_signal(
            barrier, inc=1, device_id=member(lax.rem(me + k, groups)), device_id_type=MESH
        )
        return carry

    lax.fori_loop(1, groups, greet_group, 0)
    for k in range(1, pols):
        pl.semaphore_signal(
            barrier, inc=1, device_id={"pol": lax.rem(pol_i + k, pols)}, device_id_type=MESH
        )
    pl.semaphore_wait(barrier, groups - 1 + pols - 1)

    depth = groups // rng_size
    quads = bins // STEP
    halos = SMAX // STEP
    units = chans * quads
    mid = rng_size * (depth // 2)

    def z_copy(unit, first, slot, q):
        ch, part = unit // quads, lax.rem(unit, quads)
        start = pl.multiple_of(first * bins + part * STEP, STEP)
        return pltpu.make_async_remote_copy(
            src_ref=echo.at[ch, :, pl.ds(start, STEP), :],
            dst_ref=recv.at[slot, me],
            send_sem=z_send.at[slot // units],
            recv_sem=z_recv.at[slot],
            device_id=member(q),
            device_id_type=MESH,
        )

    def own_copy(unit, first, slot):
        ch, part = unit // quads, lax.rem(unit, quads)
        start = pl.multiple_of(first * bins + part * STEP, STEP)
        return pltpu.make_async_copy(
            echo.at[ch, :, pl.ds(start, STEP), :], recv.at[slot, me], z_recv.at[slot]
        )

    def z_landed(slot):
        pltpu.make_async_copy(recv.at[slot], recv.at[slot], z_recv.at[slot]).wait()

    def place(core):
        return rng_size - 1 - core if REVERSE else core

    def send_step(step):
        def to_layer(layer, near):
            for j in range(rng_size):
                q = layer * rng_size + j
                unit = step - LAG * place(j) - FIRST * jnp.minimum(layer, 1)
                valid = (unit >= 0) & (unit < units)
                if near:

                    @pl.when(valid & (rng_i == j))
                    def _():
                        own_copy(unit, me, unit).start()

                    valid = valid & (rng_i != j)

                @pl.when(valid)
                def _():
                    z_copy(unit, q, unit, q).start()

        def send_echo(i, carry):
            gap = depth - 1 - i
            for sign in (1, -1):
                layer = pulse_i + sign * gap

                @pl.when((layer >= 0) & (layer < depth))
                def _(layer=layer):
                    to_layer(layer, False)

            return carry

        lax.fori_loop(0, depth - 1, send_echo, 0)
        to_layer(pulse_i, True)
        early = step - FIRST - RAW
        slot = units + early // quads * halos + lax.rem(early, quads)
        valid = (early >= 0) & (early < units) & (lax.rem(early, quads) < halos)
        if mid > 0:

            @pl.when(valid & (me == mid - 1))
            def _():
                own_copy(early, mid, slot).start()

            @pl.when(valid & (me != mid - 1))
            def _():
                z_copy(early, mid, slot, mid - 1).start()

    mylag = LAG * place(rng_i) + FIRST * jnp.minimum(pulse_i, 1)

    def opening(step, carry):
        send_step(step)
        return carry

    lax.fori_loop(0, AHEAD + mylag, opening, 0)

    def zero_edges():
        @pl.when(me == groups - 1)
        def _():
            spec[:, :, bins:, :, :] = jnp.zeros((chans, 2, SMAX, outer, LANES), BF16)
            quad[:, :, HALF + bins :, :, :] = jnp.zeros((4, 2, HALF, half_rows, LANES), BF16)
            quad_edge[:, :, HALF + bins :, :, :] = jnp.zeros((4, 2, HALF, 2, LANES), F32)

        @pl.when(me == 0)
        def _():
            quad[:, :, :HALF, :, :] = jnp.zeros((4, 2, HALF, half_rows, LANES), BF16)
            quad_edge[:, :, :HALF, :, :] = jnp.zeros((4, 2, HALF, 2, LANES), F32)

    zero_edges()
    for fetch in fetches:
        fetch.wait()

    per_row = LANES // outer
    for k in range(mig.shape[0]):
        for u in range(outer):
            mig_rows[u : u + 1, :] = mig[k : k + 1, u * LANES : (u + 1) * LANES].astype(F32)
        turned = mig_rows[...].T.astype(BF16)
        total = jnp.zeros((outer, LANES), F32)
        for h in range(per_row):
            total = total + jnp.dot(
                turned[h * outer : (h + 1) * outer],
                slim_t[(2 * two + h * outer) : (2 * two + (h + 1) * outer)],
                preferred_element_type=F32,
            )
        shifts[k] = total.astype(BF16)

    size = outer * LANES
    position = lax.broadcasted_iota(jnp.int32, (outer, LANES), 0) + outer * (
        lax.broadcasted_iota(jnp.int32, (outer, LANES), 1)
    )
    centred = jnp.where(position < size // 2, position, position - size).astype(F32)
    quadratic = centred * centred / size

    def phase_row(r, carry):
        turns = (0.5 * rate[r]) * quadratic
        turns = turns - jnp.round(turns)
        square = turns * turns
        cosine[r] = horner(COS_COEF, square)
        sine[r] = horner(SIN_COEF, square) * turns
        return carry

    lax.fori_loop(0, bins, phase_row, 0)

    def halo_copy(ch, part):
        return pltpu.make_async_remote_copy(
            src_ref=spec.at[ch, :, pl.ds(part * STEP, STEP)],
            dst_ref=spec.at[ch, :, pl.ds(bins + part * STEP, STEP)],
            send_sem=h_send,
            recv_sem=h_recv.at[ch, part],
            device_id=member(jnp.maximum(me - 1, 0)),
            device_id_type=MESH,
        )

    def x_copy(ch, blk, k):
        return pltpu.make_async_remote_copy(
            src_ref=image.at[ch, k - 1, :, pl.ds(blk * STEP, STEP)],
            dst_ref=quad.at[pol_i * chans + ch, :, pl.ds(HALF + blk * STEP, STEP)],
            send_sem=x_send,
            recv_sem=x_recv.at[ch, blk],
            device_id={"pol": lax.rem(pol_i + k, pols)},
            device_id_type=MESH,
        )

    def e_copy(ch, blk, k):
        return pltpu.make_async_remote_copy(
            src_ref=edge.at[ch, k - 1, :, pl.ds(blk * STEP, STEP)],
            dst_ref=quad_edge.at[pol_i * chans + ch, :, pl.ds(HALF + blk * STEP, STEP)],
            send_sem=x_send,
            recv_sem=x_recv.at[ch, blk],
            device_id={"pol": lax.rem(pol_i + k, pols)},
            device_id_type=MESH,
        )

    def drain(array, sem):
        pltpu.make_async_copy(array, array, sem).wait()

    share = 2 * STEP + 2 * STEP * 2 * 4 // (half_rows * 2)

    def landed(ch, blk):
        if pols > 1:
            drain(quad.at[pl.ds(0, pols - 1), 0, pl.ds(0, share)], x_recv.at[ch, blk])

    def relay(array, sems, recvs, chan, side):
        take = HALF if side == 0 else bins
        put = HALF + bins if side == 0 else 0
        target = jnp.maximum(me - 1, 0) if side == 0 else jnp.minimum(me + 1, groups - 1)
        return pltpu.make_async_remote_copy(
            src_ref=array.at[chan, :, pl.ds(take, HALF)],
            dst_ref=array.at[chan, :, pl.ds(put, HALF)],
            send_sem=sems.at[side],
            recv_sem=recvs.at[side],
            device_id=member(target),
            device_id_type=MESH,
        )

    sides = ((0, me > 0), (1, me < groups - 1))

    def unpack(slot):
        def body(p, carry):
            for part in range(2):
                for a in range(local_a):
                    tile = recv[slot, p, part, :, a * LANES : (a + 1) * LANES].astype(F32)
                    start = pl.multiple_of((part * outer + p * local_a + a) * STEP, STEP)
                    unpacked[pl.ds(start, STEP), :] = tile
            return carry

        lax.fori_loop(0, groups, body, 0)

    def forward(ch, g):
        rows = [unpacked[pl.ds(j, 2 * outer, stride=STEP), :] for j in range(STEP)]
        wide = jnp.concatenate([row.astype(BF16) for row in rows], axis=1)
        half = jnp.dot(first_t[...], wide, preferred_element_type=F32)
        tc, ts = twiddle[0], twiddle[1]
        turned = []
        for j in range(STEP):
            re = half[:outer, j * LANES : (j + 1) * LANES]
            im = half[outer:, j * LANES : (j + 1) * LANES]
            turned.append(
                jnp.concatenate(
                    [(re * tc + im * ts).astype(BF16), (im * tc - re * ts).astype(BF16)], axis=1
                )
            )
        done = jnp.dot(
            jnp.concatenate(turned, axis=0), fwd_t[...], preferred_element_type=F32
        ).astype(BF16)
        for j in range(STEP):
            r = g * STEP + j
            spec[ch, 0, r] = done[j * outer : (j + 1) * outer, :LANES]
            spec[ch, 1, r] = done[j * outer : (j + 1) * outer, LANES:]

    def inverse(ch, blk, g):
        amount = shifts[blk]
        turned = []
        for j in range(STEP):
            r = g * STEP + j
            re, im = spec[ch, 0, r], spec[ch, 1, r]
            for s in range(1, SMAX + 1):
                hit = amount == s
                re = jnp.where(hit, spec[ch, 0, r + s], re)
                im = jnp.where(hit, spec[ch, 1, r + s], im)
            re, im = re.astype(F32), im.astype(F32)
            c, s_ = cosine[r], sine[r]
            turned.append(
                jnp.concatenate(
                    [(re * c - im * s_).astype(BF16), (re * s_ + im * c).astype(BF16)], axis=1
                )
            )
        mid = jnp.dot(jnp.concatenate(turned, axis=0), inv_t[...], preferred_element_type=F32)
        tc, ts = twiddle[2], twiddle[3]
        columns = []
        for j in range(STEP):
            re = mid[j * outer : (j + 1) * outer, :LANES]
            im = mid[j * outer : (j + 1) * outer, LANES:]
            columns.append(
                jnp.concatenate(
                    [(re * tc - im * ts).astype(BF16), (im * tc + re * ts).astype(BF16)], axis=0
                )
            )
        done = jnp.dot(
            last_t[...], jnp.concatenate(columns, axis=1), preferred_element_type=F32
        )
        for j in range(STEP):
            for part in range(2):
                full = done[part * outer : (part + 1) * outer, j * LANES : (j + 1) * LANES]
                r = g * STEP + j
                zero = jnp.zeros((1, LANES), F32)
                rounded = full.astype(BF16)
                exact = rounded.astype(F32)
                pieces = []
                for h in range(pols):
                    low, high = h * half_rows, (h + 1) * half_rows
                    before = exact[low - 1 : low] if h > 0 else zero
                    after = exact[high : high + 1] if h < pols - 1 else zero
                    pieces.append((exact[low:high], before, after))
                for k in range(pols):
                    main, before, after = pieces[k]
                    for p in range(1, pols):
                        mine = pol_i == p
                        other = pieces[(p + k) % pols]
                        main = jnp.where(mine, other[0], main)
                        before = jnp.where(mine, other[1], before)
                        after = jnp.where(mine, other[2], after)
                    if k == 0:
                        chan = pol_i * chans + ch
                        quad[chan, part, HALF + r] = main.astype(BF16)
                        quad_edge[chan, part, HALF + r, 0:1] = before
                        quad_edge[chan, part, HALF + r, 1:2] = after
                    else:
                        image[ch, k - 1, part, r] = main.astype(BF16)
                        edge[ch, k - 1, part, r, 0:1] = before
                        edge[ch, k - 1, part, r, 1:2] = after

    def loop(count, start, fun):
        def body(i, carry):
            fun(start + i)
            return carry

        lax.fori_loop(0, count, body, 0)

    def pauli(source, target, r):
        v = [[source[c, part, r].astype(F32) for part in range(2)] for c in range(4)]
        k1 = [(v[0][i] + v[3][i]) * ROOT_HALF for i in range(2)]
        k2 = [(v[0][i] - v[3][i]) * ROOT_HALF for i in range(2)]
        k3 = [(v[1][i] + v[2][i]) * ROOT_HALF for i in range(2)]
        terms = [k[0] * k[0] + k[1] * k[1] for k in (k1, k2, k3)]
        for a, b in ((k1, k2), (k1, k3), (k2, k3)):
            terms.append(a[0] * b[0] + a[1] * b[1])
            terms.append(a[1] * b[0] - a[0] * b[1])
        for i, term in enumerate(terms):
            target[i, r] = term

    def cell_row(r):
        pauli(quad, cells, r)
        pauli(quad_edge, cells_edge, r)

    def rim_copies(ch, side, owner):
        @pl.when(sides[side][1])
        def _():
            relay(quad, r_send, r_recv, owner * chans + ch, side).start()
            relay(quad_edge, r_send, r_recv, owner * chans + ch, side).start()

    def pass_on(ch, side):
        landed(ch, rims[side])
        for k in range(side, pols):
            rim_copies(ch, side, lax.rem(pol_i + k, pols))

    def produce(ch, blk):
        inverse(ch, blk * STEP // RBLK, blk)
        for k in range(1, pols):
            e_copy(ch, blk, k).start()
            x_copy(ch, blk, k).start()

        @pl.when(blk == quads - 1)
        def _():
            rim_copies(ch, 1, pol_i)

    def take_halo(ch, part):
        @pl.when((me < groups - 1) & (me != mid - 1))
        def _():
            halo_copy(ch, part).wait_recv()

        @pl.when(me == mid - 1)
        def _():
            slot = units + ch * halos + part
            z_landed(slot)
            unpack(slot)
            forward(ch, quads + part)

    rims = (0, quads - 1)
    lagging = place(rng_i) == rng_size - 1
    leading = place(rng_i) != rng_size - 1
    prompt = lagging & (me != mid - 1)
    late = list(range(quads - halos, quads))
    for ch in range(chans):
        for part in range(quads):
            unit = ch * quads + part
            z_landed(unit)
            send_step(unit + AHEAD + mylag)
            unpack(unit)
            forward(ch, part)
            if part < halos:

                @pl.when((me > 0) & (me != mid))
                def _(ch=ch, part=part):
                    halo_copy(ch, part).start()

            if part >= halos and (part < quads - 1 or ch < chans - 1):
                produce(ch, part - halos)
            if part == quads - 1 and ch < chans - 1:

                @pl.when(prompt)
                def _(ch=ch):
                    for h in range(halos):

                        @pl.when(me < groups - 1)
                        def _(h=h):
                            halo_copy(ch, h).wait_recv()

                        produce(ch, late[h])
            if ch > 0:
                if part < halos:

                    @pl.when(jnp.logical_not(prompt))
                    def _(ch=ch, part=part):
                        take_halo(ch - 1, part)
                        produce(ch - 1, late[part])

    def range_sum(x, count):
        two = x[:-1] + x[1:]
        four = two[:-2] + two[2:]
        return four[:count] + two[4 : 4 + count] + x[6 : 6 + count]

    def component(i, low, high):
        slot, count = i % SLOTS, high - low
        tall = slice(low, high + 2 * HALF)
        for j in range(half_rows // 8):
            padded[slot, :count, 8 + j * 8 : 16 + j * 8, :] = range_sum(
                cells[i, tall, j * 8 : (j + 1) * 8, :], count
            )
        rim = range_sum(cells_edge[i, tall], count)
        padded[slot, :count, 7:8, :] = rim[:, 0:1, :]
        padded[slot, :count, 8 + half_rows : 9 + half_rows, :] = rim[:, 1:2, :]
        center = padded[slot, :count, 8 : 8 + half_rows, :]
        lane = lax.broadcasted_iota(jnp.int32, (count, half_rows, LANES), 2)
        side = jnp.where(
            lane < LANES // 2,
            padded[slot, :count, 9 : 9 + half_rows, :],
            padded[slot, :count, 7 : 7 + half_rows, :],
        )
        flat = (count * half_rows, LANES)
        both = jnp.concatenate(
            [center.reshape(flat).astype(BF16), side.reshape(flat).astype(BF16)], axis=1
        )
        total = jnp.dot(both, band[...], preferred_element_type=F32)
        total = total * (1.0 / (WIN * WIN))
        for r in range(count):
            start = (low + r) * (half_rows + 8)
            result[i, start : start + half_rows] = total[r * half_rows : (r + 1) * half_rows]

    def window(low, high):
        for i in range(9):
            component(i, low, high)

    def take_rim(side):
        @pl.when((me < groups - 1) if side == 0 else (me > 0))
        def _():
            drain(quad.at[pl.ds(0, HALF), 0, pl.ds(0, share)], r_recv.at[side])

        loop(HALF, bins + HALF if side == 0 else 0, cell_row)

    def take_quad(blk):
        landed(last, blk)
        loop(STEP, HALF + blk * STEP, cell_row)

    last = chans - 1
    inner = quads - 1 - halos

    def take_halos():
        for part in range(halos):
            take_halo(last, part)

    pl.when(lagging)(take_halos)
    produce(last, jnp.where(lagging, quads - 1, inner))
    pl.when(leading)(take_halos)
    produce(last, jnp.where(lagging, inner, quads - 1))
    for blk in late[:-1]:
        produce(last, blk)
    for ch in range(chans):
        if ch < last:
            for side in range(2):
                pass_on(ch, side)
            for blk in range(1, quads - 1):
                landed(ch, blk)
    pass_on(last, 0)
    loop(STEP, HALF, cell_row)
    early = (quads - halos) * STEP - HALF

    def take_rim_quad():
        pass_on(last, 1)
        loop(STEP, HALF + (quads - 1) * STEP, cell_row)

    @pl.when(lagging)
    def _():
        take_rim_quad()
        for blk in range(1, quads - halos):
            take_quad(blk)
        take_rim(1)
        window(0, early)
        take_rim(0)
        for blk in range(quads - halos, quads - 1):
            take_quad(blk)
        window(early, bins)

    @pl.when(leading)
    def _():
        for blk in range(1, quads - halos):
            take_quad(blk)
        take_rim_quad()
        for blk in range(quads - halos, quads - 1):
            take_quad(blk)
        window(HALF, bins - HALF)
        take_rim(0)
        window(bins - HALF, bins)
        take_rim(1)
        window(0, HALF)

    for i in range(9):
        for a in range(half_rows):
            piece = result[i, pl.ds(a, bins, stride=half_rows + 8), :]
            out[i, :, a * LANES : (a + 1) * LANES] = piece.astype(BF16)

    drain(recv.at[pl.ds(0, units), pl.ds(0, groups - 1)], z_send.at[0])

    @pl.when(me != mid - 1)
    def _():
        drain(recv.at[pl.ds(0, chans * halos), 0], z_send.at[1])

    @pl.when((me > 0) & (me != mid))
    def _():
        drain(spec.at[:, :, pl.ds(0, SMAX)], h_send)

    if pols > 1:
        rows = pl.ds(0, share * bins // (2 * STEP))
        drain(quad.at[pl.ds(0, chans * (pols - 1)), :, rows], x_send)
    for side, cond in sides:

        @pl.when(cond)
        def _(side=side):
            drain(quad.at[pl.ds(0, HALF), 0, pl.ds(0, share)], r_send.at[side])


def shards(echoes, migration, fm_rate):
    rng_size = lax.axis_size("rng")
    groups = lax.axis_size("pulse") * rng_size
    pols = lax.axis_size("pol")
    chans = echoes.shape[0]
    pulses = echoes.shape[3]
    bins = echoes.shape[2] // groups
    outer = groups * pulses // LANES
    half_rows = outer // pols
    units = chans * (bins // STEP)
    consts = tables(outer)
    vmem = pl.BlockSpec(memory_space=pltpu.VMEM)
    anywhere = pl.BlockSpec(memory_space=pltpu.HBM)
    dma = pltpu.SemaphoreType.DMA
    tall = bins + 2 * HALF
    return pl.pallas_call(
        functools.partial(kernel, chans, groups, pols, bins, outer, rng_size),
        out_shape=pltpu.VMEM((9, bins, half_rows * LANES), BF16),
        in_specs=[
            anywhere,
            anywhere,
            pl.BlockSpec(memory_space=pltpu.SMEM),
        ]
        + [anywhere] * len(consts),
        out_specs=vmem,
        scratch_shapes=[
            pltpu.VMEM(migration.shape, jnp.int32),
            *(pltpu.VMEM(table.shape, table.dtype) for table in consts),
            dma((1 + len(consts),)),
            pltpu.VMEM((units + chans * (SMAX // STEP), groups, 2, STEP, pulses), BF16),
            pltpu.VMEM((2 * outer * STEP, LANES), F32),
            pltpu.VMEM((chans, 2, bins + SMAX, outer, LANES), BF16),
            pltpu.VMEM((chans, pols - 1, 2, bins, half_rows, LANES), BF16),
            pltpu.VMEM((chans, pols - 1, 2, bins, 2, LANES), F32),
            pltpu.VMEM((4, 2, tall, half_rows, LANES), BF16),
            pltpu.VMEM((4, 2, tall, 2, LANES), F32),
            pltpu.VMEM((migration.shape[0], outer, LANES), BF16),
            pltpu.VMEM((outer, LANES), F32),
            pltpu.VMEM((bins, outer, LANES), F32),
            pltpu.VMEM((bins, outer, LANES), F32),
            pltpu.VMEM((9, tall, half_rows, LANES), F32),
            pltpu.VMEM((9, tall, 2, LANES), F32),
            pltpu.VMEM((SLOTS, bins, half_rows + 16, LANES), F32),
            pltpu.VMEM((9, bins * (half_rows + 8), LANES), F32),
            dma((2,)),
            dma((units + chans * (SMAX // STEP),)),
            dma,
            dma((chans, SMAX // STEP)),
            dma,
            dma((chans, bins // STEP)),
            dma((2,)),
            dma((2,)),
        ],
        compiler_params=pltpu.CompilerParams(
            collective_id=0, has_side_effects=True, vmem_limit_bytes=58 * 1024 * 1024
        ),
    )(echoes, migration, fm_rate, *consts)


def solution(mesh):
    placed = (
        P(("scene", "pol"), None, None, ("pulse", "rng")),
        P(("scene", "pulse", "rng"), None),
        P(("scene", "pulse", "rng")),
    )
    return jax.shard_map(
        shards,
        mesh=mesh,
        in_specs=placed,
        out_specs=P(None, ("scene", "pulse", "rng"), "pol"),
        check_vma=False,
    )
```

```python
import functools
import math

import jax
import jax.numpy as jnp
import numpy as np
from jax import lax
from jax.experimental import pallas as pl
from jax.experimental.pallas import tpu as pltpu
from jax.sharding import PartitionSpec as P

RBLK = 8
SMAX = 8
WIN = 7
HALF = WIN // 2
LANES = 128
STEP = 4
SLOTS = 3
AHEAD = 3
LAG = 2
FIRST = 0
RAW = 5
REVERSE = False
ROOT_HALF = 0.7071067811865476
MESH = pl.DeviceIdType.MESH
F32 = jnp.float32
BF16 = jnp.bfloat16


def fit(function, degree):
    nodes = (np.cos(np.pi * (np.arange(64) + 0.5) / 64) + 1) / 8
    poly = np.polynomial.Chebyshev.fit(nodes, function(nodes), degree, domain=[0, 0.25])
    return [float(v) for v in poly.convert(kind=np.polynomial.Polynomial).coef]


SIN_COEF = fit(lambda y: np.sin(2 * np.pi * np.sqrt(y)) / np.sqrt(y), 7)
COS_COEF = fit(lambda y: np.cos(2 * np.pi * np.sqrt(y)), 7)


def horner(coefs, y):
    total = jnp.full_like(y, coefs[-1])
    for coef in coefs[-2::-1]:
        total = total * y + coef
    return total


def trig(period, height, width):
    index = np.arange(height)[:, None] * np.arange(width)[None, :] % period
    return np.cos(2 * np.pi * index / period), np.sin(2 * np.pi * index / period)


def tables(outer):
    size = outer * LANES
    oc, os_ = trig(outer, outer, outer)
    scale = 1.0 / math.sqrt(outer)
    first = np.block([[oc, os_], [-os_, oc]]) * scale
    last = np.block([[oc, -os_], [os_, oc]]) * scale
    ic, is_ = trig(LANES, LANES, LANES)
    fwd = np.block([[ic, -is_], [is_, ic]])
    inv = np.block([[ic, is_], [-is_, ic]])
    tc, ts = trig(size, outer, LANES)
    row = np.arange(LANES)
    gap = row[:, None] - row[None, :]
    near = np.abs(gap) <= HALF
    wrap = np.abs(np.abs(gap) - LANES) <= HALF
    band = np.concatenate([near, wrap], axis=0)
    per_row = LANES // outer
    spread = np.zeros((per_row * outer, LANES))
    for u in range(outer):
        for h in range(per_row):
            spread[h * outer + u, per_row * u + h] = 1
    short = lambda v: np.asarray(v, np.float32).astype(BF16).astype(np.float32)

    def gain(v):
        return float(np.sum(v * short(v)) / np.sum(v * v))

    root = math.sqrt(LANES)
    there, back = root * gain(first) * gain(fwd), root * gain(inv) * gain(last)
    twiddle = np.stack([tc / there, ts / there, tc / back, ts / back])
    fill = lambda v, width: np.pad(v, ((0, 0), (0, width - v.shape[1])))
    slim = np.concatenate([fill(first, LANES), fill(last, LANES), spread])
    wide = np.concatenate([fwd, inv, fill(band, 2 * LANES)])
    return jnp.asarray(wide, BF16), jnp.asarray(slim, BF16), jnp.asarray(twiddle, F32)


def edge_rows(pols):
    return 1 if pols == 2 else 2


def kernel(
    chans, groups, pols, bins, outer, rng_size,
    echo, mig_hbm, rate, wide_hbm, slim_hbm, twiddle_hbm,
    out,
    mig, wide_t, slim_t, twiddle, t_sem,
    recv, unpacked, spec, image, edge, quad, quad_edge, shifts, mig_rows, cosine, sine,
    cells, cells_edge, padded, result,
    z_send, z_recv, h_send, h_recv, x_send, x_recv, e_send, r_send, r_recv,
):
    half_rows = outer // pols
    rows_out = edge_rows(pols)
    local_a = outer // groups
    pulse_i, rng_i, pol_i = (lax.axis_index(n) for n in ("pulse", "rng", "pol"))
    me = pulse_i * rng_size + rng_i

    def member(q):
        return {"pulse": q // rng_size, "rng": lax.rem(q, rng_size)}

    fetches = [
        pltpu.make_async_copy(source, target, t_sem.at[i])
        for i, (source, target) in enumerate(
            ((mig_hbm, mig), (slim_hbm, slim_t), (twiddle_hbm, twiddle), (wide_hbm, wide_t))
        )
    ]
    two = 2 * outer
    first_t, last_t = slim_t.at[0:two, 0:two], slim_t.at[two : 2 * two, 0:two]
    fwd_t, inv_t = wide_t.at[0 : 2 * LANES], wide_t.at[2 * LANES : 4 * LANES]
    band = wide_t.at[4 * LANES : 6 * LANES, 0:LANES]

    barrier = pltpu.get_barrier_semaphore()

    def greet_group(k, carry):
        pl.semaphore_signal(
            barrier, inc=1, device_id=member(lax.rem(me + k, groups)), device_id_type=MESH
        )
        return carry

    lax.fori_loop(1, groups, greet_group, 0)
    for k in range(1, pols):
        pl.semaphore_signal(
            barrier, inc=1, device_id={"pol": lax.rem(pol_i + k, pols)}, device_id_type=MESH
        )
    for fetch in fetches:
        fetch.start()
    pl.semaphore_wait(barrier, groups - 1 + pols - 1)

    depth = groups // rng_size
    quads = bins // STEP
    halos = SMAX // STEP
    units = chans * quads
    mid = rng_size * (depth // 2)

    def z_copy(unit, first, slot, q):
        ch, part = unit // quads, lax.rem(unit, quads)
        start = pl.multiple_of(first * bins + part * STEP, STEP)
        return pltpu.make_async_remote_copy(
            src_ref=echo.at[ch, :, pl.ds(start, STEP), :],
            dst_ref=recv.at[slot, me],
            send_sem=z_send.at[slot // units],
            recv_sem=z_recv.at[slot],
            device_id=member(q),
            device_id_type=MESH,
        )

    def own_copy(unit, first, slot):
        ch, part = unit // quads, lax.rem(unit, quads)
        start = pl.multiple_of(first * bins + part * STEP, STEP)
        return pltpu.make_async_copy(
            echo.at[ch, :, pl.ds(start, STEP), :], recv.at[slot, me], z_recv.at[slot]
        )

    def z_landed(slot):
        pltpu.make_async_copy(recv.at[slot], recv.at[slot], z_recv.at[slot]).wait()

    def place(core):
        return rng_size - 1 - core if REVERSE else core

    def send_step(step):
        def to_layer(layer, near):
            for j in range(rng_size):
                q = layer * rng_size + j
                unit = step - LAG * place(j) - FIRST * jnp.minimum(layer, 1)
                valid = (unit >= 0) & (unit < units)
                if near:

                    @pl.when(valid & (rng_i == j))
                    def _():
                        own_copy(unit, me, unit).start()

                    valid = valid & (rng_i != j)

                @pl.when(valid)
                def _():
                    z_copy(unit, q, unit, q).start()

        def send_echo(i, carry):
            gap = depth - 1 - i
            for sign in (1, -1):
                layer = pulse_i + sign * gap

                @pl.when((layer >= 0) & (layer < depth))
                def _(layer=layer):
                    to_layer(layer, False)

            return carry

        lax.fori_loop(0, depth - 1, send_echo, 0)
        to_layer(pulse_i, True)
        early = step - FIRST - RAW
        slot = units + early // quads * halos + lax.rem(early, quads)
        valid = (early >= 0) & (early < units) & (lax.rem(early, quads) < halos)
        if mid > 0:

            @pl.when(valid & (me == mid - 1))
            def _():
                own_copy(early, mid, slot).start()

            @pl.when(valid & (me != mid - 1))
            def _():
                z_copy(early, mid, slot, mid - 1).start()

    mylag = LAG * place(rng_i) + FIRST * jnp.minimum(pulse_i, 1)

    def opening(step, carry):
        send_step(step)
        return carry

    lax.fori_loop(0, AHEAD + mylag, opening, 0)

    def zero_edges():
        @pl.when(me == groups - 1)
        def _():
            spec[:, :, bins:, :, :] = jnp.zeros((chans, 2, SMAX, outer, LANES), BF16)
            quad[:, :, HALF + bins :, :, :] = jnp.zeros((4, 2, HALF, half_rows, LANES), BF16)
            quad_edge[:, :, HALF + bins :, :, :] = jnp.zeros((4, 2, HALF, rows_out, LANES), F32)

        @pl.when(me == 0)
        def _():
            quad[:, :, :HALF, :, :] = jnp.zeros((4, 2, HALF, half_rows, LANES), BF16)
            quad_edge[:, :, :HALF, :, :] = jnp.zeros((4, 2, HALF, rows_out, LANES), F32)

    zero_edges()
    for fetch in fetches:
        fetch.wait()

    per_row = LANES // outer
    for k in range(mig.shape[0]):
        for u in range(outer):
            mig_rows[u : u + 1, :] = mig[k : k + 1, u * LANES : (u + 1) * LANES].astype(F32)
        turned = mig_rows[...].T.astype(BF16)
        total = jnp.zeros((outer, LANES), F32)
        for h in range(per_row):
            total = total + jnp.dot(
                turned[h * outer : (h + 1) * outer],
                slim_t[(2 * two + h * outer) : (2 * two + (h + 1) * outer)],
                preferred_element_type=F32,
            )
        shifts[k] = total.astype(BF16)

    size = outer * LANES
    position = lax.broadcasted_iota(jnp.int32, (outer, LANES), 0) + outer * (
        lax.broadcasted_iota(jnp.int32, (outer, LANES), 1)
    )
    centred = jnp.where(position < size // 2, position, position - size).astype(F32)
    quadratic = centred * centred / size

    def phase_row(r, carry):
        turns = (0.5 * rate[r]) * quadratic
        turns = turns - jnp.round(turns)
        square = turns * turns
        cosine[r] = horner(COS_COEF, square)
        sine[r] = horner(SIN_COEF, square) * turns
        return carry

    lax.fori_loop(0, bins, phase_row, 0)

    def halo_copy(ch, part):
        return pltpu.make_async_remote_copy(
            src_ref=spec.at[ch, :, pl.ds(part * STEP, STEP)],
            dst_ref=spec.at[ch, :, pl.ds(bins + part * STEP, STEP)],
            send_sem=h_send,
            recv_sem=h_recv.at[ch, part],
            device_id=member(jnp.maximum(me - 1, 0)),
            device_id_type=MESH,
        )

    def x_copy(ch, blk, k):
        return pltpu.make_async_remote_copy(
            src_ref=image.at[ch, k - 1, :, pl.ds(blk * STEP, STEP)],
            dst_ref=quad.at[pol_i * chans + ch, :, pl.ds(HALF + blk * STEP, STEP)],
            send_sem=x_send,
            recv_sem=x_recv.at[ch, blk],
            device_id={"pol": lax.rem(pol_i + k, pols)},
            device_id_type=MESH,
        )

    def e_copy(ch, blk, k):
        return pltpu.make_async_remote_copy(
            src_ref=edge.at[ch, k - 1, :, pl.ds(blk * STEP, STEP)],
            dst_ref=quad_edge.at[pol_i * chans + ch, :, pl.ds(HALF + blk * STEP, STEP)],
            send_sem=e_send,
            recv_sem=x_recv.at[ch, blk],
            device_id={"pol": lax.rem(pol_i + k, pols)},
            device_id_type=MESH,
        )

    def drain(array, sem):
        pltpu.make_async_copy(array, array, sem).wait()

    share = 2 * STEP * half_rows // 16 + 2 * STEP * rows_out * 4 // (16 * 2)
    part_row = pl.ds(0, 16)

    def landed(ch, blk):
        if pols > 1:
            drain(quad.at[pl.ds(0, pols - 1), 0, pl.ds(0, share), part_row], x_recv.at[ch, blk])

    def relay(array, sems, recvs, chan, side):
        take = HALF if side == 0 else bins
        put = HALF + bins if side == 0 else 0
        target = jnp.maximum(me - 1, 0) if side == 0 else jnp.minimum(me + 1, groups - 1)
        return pltpu.make_async_remote_copy(
            src_ref=array.at[chan, :, pl.ds(take, HALF)],
            dst_ref=array.at[chan, :, pl.ds(put, HALF)],
            send_sem=sems.at[side],
            recv_sem=recvs.at[side],
            device_id=member(target),
            device_id_type=MESH,
        )

    sides = ((0, me > 0), (1, me < groups - 1))

    def unpack(slot):
        def body(p, carry):
            for part in range(2):
                for a in range(local_a):
                    tile = recv[slot, p, part, :, a * LANES : (a + 1) * LANES].astype(F32)
                    start = pl.multiple_of((part * outer + p * local_a + a) * STEP, STEP)
                    unpacked[pl.ds(start, STEP), :] = tile
            return carry

        lax.fori_loop(0, groups, body, 0)

    def forward(ch, g):
        rows = [unpacked[pl.ds(j, 2 * outer, stride=STEP), :] for j in range(STEP)]
        wide = jnp.concatenate([row.astype(BF16) for row in rows], axis=1)
        half = jnp.dot(first_t[...], wide, preferred_element_type=F32)
        tc, ts = twiddle[0], twiddle[1]
        turned = []
        for j in range(STEP):
            re = half[:outer, j * LANES : (j + 1) * LANES]
            im = half[outer:, j * LANES : (j + 1) * LANES]
            turned.append(
                jnp.concatenate(
                    [(re * tc + im * ts).astype(BF16), (im * tc - re * ts).astype(BF16)], axis=1
                )
            )
        done = jnp.dot(
            jnp.concatenate(turned, axis=0), fwd_t[...], preferred_element_type=F32
        ).astype(BF16)
        for j in range(STEP):
            r = g * STEP + j
            spec[ch, 0, r] = done[j * outer : (j + 1) * outer, :LANES]
            spec[ch, 1, r] = done[j * outer : (j + 1) * outer, LANES:]

    def inverse(ch, blk, g):
        amount = shifts[blk]
        turned = []
        for j in range(STEP):
            r = g * STEP + j
            re, im = spec[ch, 0, r], spec[ch, 1, r]
            for s in range(1, SMAX + 1):
                hit = amount == s
                re = jnp.where(hit, spec[ch, 0, r + s], re)
                im = jnp.where(hit, spec[ch, 1, r + s], im)
            re, im = re.astype(F32), im.astype(F32)
            c, s_ = cosine[r], sine[r]
            turned.append(
                jnp.concatenate(
                    [(re * c - im * s_).astype(BF16), (re * s_ + im * c).astype(BF16)], axis=1
                )
            )
        mid = jnp.dot(jnp.concatenate(turned, axis=0), inv_t[...], preferred_element_type=F32)
        tc, ts = twiddle[2], twiddle[3]
        columns = []
        for j in range(STEP):
            re = mid[j * outer : (j + 1) * outer, :LANES]
            im = mid[j * outer : (j + 1) * outer, LANES:]
            columns.append(
                jnp.concatenate(
                    [(re * tc - im * ts).astype(BF16), (im * tc + re * ts).astype(BF16)], axis=0
                )
            )
        done = jnp.dot(
            last_t[...], jnp.concatenate(columns, axis=1), preferred_element_type=F32
        )
        for j in range(STEP):
            for part in range(2):
                full = done[part * outer : (part + 1) * outer, j * LANES : (j + 1) * LANES]
                r = g * STEP + j
                zero = jnp.zeros((1, LANES), F32)
                rounded = full.astype(BF16)
                exact = rounded.astype(F32)
                pieces = []
                for h in range(pols):
                    low, high = h * half_rows, (h + 1) * half_rows
                    before = exact[low - 1 : low] if h > 0 else zero
                    after = exact[high : high + 1] if h < pols - 1 else zero
                    outside = [before, after]
                    if rows_out == 1:
                        outside = [after if h == 0 else before]
                    pieces.append([exact[low:high]] + outside)
                for k in range(pols):
                    main, *outside = pieces[k]
                    for p in range(1, pols):
                        mine = pol_i == p
                        other = pieces[(p + k) % pols]
                        main = jnp.where(mine, other[0], main)
                        outside = [jnp.where(mine, o, v) for o, v in zip(other[1:], outside)]
                    if k == 0:
                        chan = pol_i * chans + ch
                        quad[chan, part, HALF + r] = main.astype(BF16)
                        for n, row in enumerate(outside):
                            quad_edge[chan, part, HALF + r, n : n + 1] = row
                    else:
                        image[ch, k - 1, part, r] = main.astype(BF16)
                        for n, row in enumerate(outside):
                            edge[ch, k - 1, part, r, n : n + 1] = row

    def loop(count, start, fun):
        def body(i, carry):
            fun(start + i)
            return carry

        lax.fori_loop(0, count, body, 0)

    def pauli(source, target, r):
        v = [[source[c, part, r].astype(F32) for part in range(2)] for c in range(4)]
        k1 = [(v[0][i] + v[3][i]) * ROOT_HALF for i in range(2)]
        k2 = [(v[0][i] - v[3][i]) * ROOT_HALF for i in range(2)]
        k3 = [(v[1][i] + v[2][i]) * ROOT_HALF for i in range(2)]
        terms = [k[0] * k[0] + k[1] * k[1] for k in (k1, k2, k3)]
        for a, b in ((k1, k2), (k1, k3), (k2, k3)):
            terms.append(a[0] * b[0] + a[1] * b[1])
            terms.append(a[1] * b[0] - a[0] * b[1])
        for i, term in enumerate(terms):
            target[i, r] = term

    def cell_row(r):
        pauli(quad, cells, r)
        pauli(quad_edge, cells_edge, r)

    def rim_copies(ch, side, owner):
        @pl.when(sides[side][1])
        def _():
            relay(quad, r_send, r_recv, owner * chans + ch, side).start()
            relay(quad_edge, r_send, r_recv, owner * chans + ch, side).start()

    def pass_on(ch, side):
        landed(ch, rims[side])
        for k in range(side, pols):
            rim_copies(ch, side, lax.rem(pol_i + k, pols))

    def produce(ch, blk):
        inverse(ch, blk * STEP // RBLK, blk)
        for k in range(1, pols):
            e_copy(ch, blk, k).start()
            x_copy(ch, blk, k).start()
        if blk == quads - 1:
            rim_copies(ch, 1, pol_i)

    def take_halo(ch, part):
        @pl.when((me < groups - 1) & (me != mid - 1))
        def _():
            halo_copy(ch, part).wait_recv()

        @pl.when(me == mid - 1)
        def _():
            slot = units + ch * halos + part
            z_landed(slot)
            unpack(slot)
            forward(ch, quads + part)

    rims = (0, quads - 1)
    lagging = place(rng_i) == rng_size - 1
    leading = place(rng_i) != rng_size - 1
    prompt = lagging & (me != mid - 1)
    late = list(range(quads - halos, quads))
    for ch in range(chans):
        for part in range(quads):
            unit = ch * quads + part
            z_landed(unit)
            send_step(unit + AHEAD + mylag)
            unpack(unit)
            forward(ch, part)
            if part < halos:

                @pl.when((me > 0) & (me != mid))
                def _(ch=ch, part=part):
                    halo_copy(ch, part).start()

            if part >= halos and (part < quads - 1 or ch < chans - 1):
                produce(ch, part - halos)
            if part == quads - 1 and ch < chans - 1:

                @pl.when(prompt)
                def _(ch=ch):
                    for h in range(halos):

                        @pl.when(me < groups - 1)
                        def _(h=h):
                            halo_copy(ch, h).wait_recv()

                        produce(ch, late[h])
            if ch > 0:
                if part < halos:

                    @pl.when(jnp.logical_not(prompt))
                    def _(ch=ch, part=part):
                        take_halo(ch - 1, part)
                        produce(ch - 1, late[part])

    def range_sum(x, count):
        two = x[:-1] + x[1:]
        four = two[:-2] + two[2:]
        return four[:count] + two[4 : 4 + count] + x[6 : 6 + count]

    def component(i, low, high):
        slot, count = i % SLOTS, high - low
        tall = slice(low, high + 2 * HALF)
        for j in range(half_rows // 8):
            padded[slot, :count, 8 + j * 8 : 16 + j * 8, :] = range_sum(
                cells[i, tall, j * 8 : (j + 1) * 8, :], count
            )
        rim = range_sum(cells_edge[i, tall], count)
        before, after = rim[:, 0:1, :], rim[:, rows_out - 1 :, :]
        if rows_out == 1:
            before = jnp.where(pol_i == 0, 0.0, before)
            after = jnp.where(pol_i == 0, after, 0.0)
        padded[slot, :count, 7:8, :] = before
        padded[slot, :count, 8 + half_rows : 9 + half_rows, :] = after
        center = padded[slot, :count, 8 : 8 + half_rows, :]
        lane = lax.broadcasted_iota(jnp.int32, (count, half_rows, LANES), 2)
        side = jnp.where(
            lane < LANES // 2,
            padded[slot, :count, 9 : 9 + half_rows, :],
            padded[slot, :count, 7 : 7 + half_rows, :],
        )
        flat = (count * half_rows, LANES)
        both = jnp.concatenate(
            [center.reshape(flat).astype(BF16), side.reshape(flat).astype(BF16)], axis=1
        )
        total = jnp.dot(both, band[...], preferred_element_type=F32)
        total = total * (1.0 / (WIN * WIN))
        for r in range(count):
            start = (low + r) * (half_rows + 8)
            result[i, start : start + half_rows] = total[r * half_rows : (r + 1) * half_rows]

    def gather(i):
        for a in range(half_rows):
            piece = result[i, pl.ds(a, bins, stride=half_rows + 8), :]
            out[i, :, a * LANES : (a + 1) * LANES] = piece.astype(BF16)

    def window(low, high, finish=False):
        for i in range(9):
            component(i, low, high)
            if finish and i > 0:
                gather(i - 1)
        if finish:
            gather(8)

    def take_rim(side):
        @pl.when((me < groups - 1) if side == 0 else (me > 0))
        def _():
            drain(quad.at[pl.ds(0, HALF), 0, pl.ds(0, share), part_row], r_recv.at[side])

        loop(HALF, bins + HALF if side == 0 else 0, cell_row)

    def take_quad(blk):
        landed(last, blk)
        loop(STEP, HALF + blk * STEP, cell_row)

    last = chans - 1
    inner = quads - 1 - halos

    def take_halos():
        for part in range(halos):
            take_halo(last, part)

    produce(last, inner)
    take_halos()
    produce(last, quads - 1)
    for blk in late[:-1]:
        produce(last, blk)
    for ch in range(chans):
        if ch < last:
            for side in range(2):
                pass_on(ch, side)
            for blk in range(1, quads - 1):
                landed(ch, blk)
    pass_on(last, 0)
    loop(STEP, HALF, cell_row)
    early = (quads - halos) * STEP - HALF

    def take_rim_quad():
        pass_on(last, 1)
        loop(STEP, HALF + (quads - 1) * STEP, cell_row)

    @pl.when(lagging)
    def _():
        for blk in range(1, quads - halos):
            take_quad(blk)
        take_rim(1)
        window(0, early)
        take_rim_quad()
        take_rim(0)
        for blk in range(quads - halos, quads - 1):
            take_quad(blk)
        window(early, bins, True)

    @pl.when(leading)
    def _():
        for blk in range(1, quads - halos):
            take_quad(blk)
        take_rim_quad()
        for blk in range(quads - halos, quads - 1):
            take_quad(blk)
        window(HALF, bins - HALF)
        take_rim(0)
        window(bins - HALF, bins)
        take_rim(1)
        window(0, HALF, True)

    drain(recv.at[pl.ds(0, units), pl.ds(0, groups - 1)], z_send.at[0])

    @pl.when(me != mid - 1)
    def _():
        drain(recv.at[pl.ds(0, chans * halos), 0], z_send.at[1])

    @pl.when((me > 0) & (me != mid))
    def _():
        drain(spec.at[:, :, pl.ds(0, SMAX)], h_send)

    if pols > 1:
        drain(image, x_send)
        drain(edge, e_send)
    for side, cond in sides:

        @pl.when(cond)
        def _(side=side):
            drain(quad.at[pl.ds(0, HALF), 0, pl.ds(0, share), part_row], r_send.at[side])


def shards(echoes, migration, fm_rate):
    rng_size = lax.axis_size("rng")
    groups = lax.axis_size("pulse") * rng_size
    pols = lax.axis_size("pol")
    chans = echoes.shape[0]
    pulses = echoes.shape[3]
    bins = echoes.shape[2] // groups
    outer = groups * pulses // LANES
    half_rows = outer // pols
    units = chans * (bins // STEP)
    consts = tables(outer)
    vmem = pl.BlockSpec(memory_space=pltpu.VMEM)
    anywhere = pl.BlockSpec(memory_space=pltpu.HBM)
    dma = pltpu.SemaphoreType.DMA
    tall = bins + 2 * HALF
    return pl.pallas_call(
        functools.partial(kernel, chans, groups, pols, bins, outer, rng_size),
        out_shape=pltpu.VMEM((9, bins, half_rows * LANES), BF16),
        in_specs=[
            anywhere,
            anywhere,
            pl.BlockSpec(memory_space=pltpu.SMEM),
        ]
        + [anywhere] * len(consts),
        out_specs=vmem,
        scratch_shapes=[
            pltpu.VMEM(migration.shape, jnp.int32),
            *(pltpu.VMEM(table.shape, table.dtype) for table in consts),
            dma((1 + len(consts),)),
            pltpu.VMEM((units + chans * (SMAX // STEP), groups, 2, STEP, pulses), BF16),
            pltpu.VMEM((2 * outer * STEP, LANES), F32),
            pltpu.VMEM((chans, 2, bins + SMAX, outer, LANES), BF16),
            pltpu.VMEM((chans, pols - 1, 2, bins, half_rows, LANES), BF16),
            pltpu.VMEM((chans, pols - 1, 2, bins, edge_rows(pols), LANES), F32),
            pltpu.VMEM((4, 2, tall, half_rows, LANES), BF16),
            pltpu.VMEM((4, 2, tall, edge_rows(pols), LANES), F32),
            pltpu.VMEM((migration.shape[0], outer, LANES), BF16),
            pltpu.VMEM((outer, LANES), F32),
            pltpu.VMEM((bins, outer, LANES), F32),
            pltpu.VMEM((bins, outer, LANES), F32),
            pltpu.VMEM((9, tall, half_rows, LANES), F32),
            pltpu.VMEM((9, tall, edge_rows(pols), LANES), F32),
            pltpu.VMEM((SLOTS, bins, half_rows + 16, LANES), F32),
            pltpu.VMEM((9, bins * (half_rows + 8), LANES), F32),
            dma((2,)),
            dma((units + chans * (SMAX // STEP),)),
            dma,
            dma((chans, SMAX // STEP)),
            dma,
            dma((chans, bins // STEP)),
            dma,
            dma((2,)),
            dma((2,)),
        ],
        compiler_params=pltpu.CompilerParams(
            collective_id=0, has_side_effects=True, vmem_limit_bytes=58 * 1024 * 1024
        ),
    )(echoes, migration, fm_rate, *consts)


def solution(mesh):
    placed = (
        P(("scene", "pol"), None, None, ("pulse", "rng")),
        P(("scene", "pulse", "rng"), None),
        P(("scene", "pulse", "rng")),
    )
    return jax.shard_map(
        shards,
        mesh=mesh,
        in_specs=placed,
        out_specs=P(None, ("scene", "pulse", "rng"), "pol"),
        check_vma=False,
    )
```

```python
import functools
import math

import jax
import jax.numpy as jnp
import numpy as np
from jax import lax
from jax.experimental import pallas as pl
from jax.experimental.pallas import tpu as pltpu
from jax.sharding import PartitionSpec as P

RBLK = 8
SMAX = 8
WIN = 7
HALF = WIN // 2
LANES = 128
STEP = 4
SLOTS = 3
AHEAD = 3
LAG = 2
FIRST = 0
RAW = 5
REVERSE = False
ROOT_HALF = 0.7071067811865476
MESH = pl.DeviceIdType.MESH
F32 = jnp.float32
BF16 = jnp.bfloat16


def fit(function, degree):
    nodes = (np.cos(np.pi * (np.arange(64) + 0.5) / 64) + 1) / 8
    poly = np.polynomial.Chebyshev.fit(nodes, function(nodes), degree, domain=[0, 0.25])
    return [float(v) for v in poly.convert(kind=np.polynomial.Polynomial).coef]


SIN_COEF = fit(lambda y: np.sin(2 * np.pi * np.sqrt(y)) / np.sqrt(y), 7)
COS_COEF = fit(lambda y: np.cos(2 * np.pi * np.sqrt(y)), 7)


def horner(coefs, y):
    total = jnp.full_like(y, coefs[-1])
    for coef in coefs[-2::-1]:
        total = total * y + coef
    return total


def trig(period, height, width):
    index = np.arange(height)[:, None] * np.arange(width)[None, :] % period
    return np.cos(2 * np.pi * index / period), np.sin(2 * np.pi * index / period)


def tables(outer):
    size = outer * LANES
    oc, os_ = trig(outer, outer, outer)
    scale = 1.0 / math.sqrt(outer)
    first = np.block([[oc, os_], [-os_, oc]]) * scale
    last = np.block([[oc, -os_], [os_, oc]]) * scale
    ic, is_ = trig(LANES, LANES, LANES)
    fwd = np.block([[ic, -is_], [is_, ic]])
    inv = np.block([[ic, is_], [-is_, ic]])
    tc, ts = trig(size, outer, LANES)
    row = np.arange(LANES)
    gap = row[:, None] - row[None, :]
    near = np.abs(gap) <= HALF
    wrap = np.abs(np.abs(gap) - LANES) <= HALF
    band = np.concatenate([near, wrap], axis=0)
    per_row = LANES // outer
    spread = np.zeros((per_row * outer, LANES))
    for u in range(outer):
        for h in range(per_row):
            spread[h * outer + u, per_row * u + h] = 1
    short = lambda v: np.asarray(v, np.float32).astype(BF16).astype(np.float32)

    def gain(v):
        return float(np.sum(v * short(v)) / np.sum(v * v))

    root = math.sqrt(LANES)
    there, back = root * gain(first) * gain(fwd), root * gain(inv) * gain(last)
    twiddle = np.stack([tc / there, ts / there, tc / back, ts / back])
    fill = lambda v, width: np.pad(v, ((0, 0), (0, width - v.shape[1])))
    slim = np.concatenate([fill(first, LANES), fill(last, LANES), spread])
    wide = np.concatenate([fwd, inv, fill(band, 2 * LANES)])
    return jnp.asarray(wide, BF16), jnp.asarray(slim, BF16), jnp.asarray(twiddle, F32)


def edge_rows(pols):
    return 1 if pols == 2 else 2


def kernel(
    chans, groups, pols, bins, outer, rng_size,
    echo, mig_hbm, rate, wide_hbm, slim_hbm, twiddle_hbm,
    out,
    mig, wide_t, slim_t, twiddle, t_sem,
    recv, unpacked, spec, image, edge, quad, quad_edge, shifts, mig_rows, cosine, sine,
    cells, cells_edge, padded, result,
    z_send, z_recv, h_send, h_recv, x_send, x_recv, e_send, r_send, r_recv,
):
    half_rows = outer // pols
    rows_out = edge_rows(pols)
    local_a = outer // groups
    pulse_i, rng_i, pol_i = (lax.axis_index(n) for n in ("pulse", "rng", "pol"))
    me = pulse_i * rng_size + rng_i

    def member(q):
        return {"pulse": q // rng_size, "rng": lax.rem(q, rng_size)}

    fetches = [
        pltpu.make_async_copy(source, target, t_sem.at[i])
        for i, (source, target) in enumerate(
            ((mig_hbm, mig), (slim_hbm, slim_t), (twiddle_hbm, twiddle), (wide_hbm, wide_t))
        )
    ]
    two = 2 * outer
    first_t, last_t = slim_t.at[0:two, 0:two], slim_t.at[two : 2 * two, 0:two]
    fwd_t, inv_t = wide_t.at[0 : 2 * LANES], wide_t.at[2 * LANES : 4 * LANES]
    band = wide_t.at[4 * LANES : 6 * LANES, 0:LANES]

    barrier = pltpu.get_barrier_semaphore()

    def greet_group(k, carry):
        pl.semaphore_signal(
            barrier, inc=1, device_id=member(lax.rem(me + k, groups)), device_id_type=MESH
        )
        return carry

    lax.fori_loop(1, groups, greet_group, 0)
    for k in range(1, pols):
        pl.semaphore_signal(
            barrier, inc=1, device_id={"pol": lax.rem(pol_i + k, pols)}, device_id_type=MESH
        )
    for fetch in fetches:
        fetch.start()
    pl.semaphore_wait(barrier, groups - 1 + pols - 1)

    depth = groups // rng_size
    quads = bins // STEP
    halos = SMAX // STEP
    units = chans * quads
    mid = rng_size * (depth // 2)

    def z_copy(unit, first, slot, q):
        ch, part = unit // quads, lax.rem(unit, quads)
        start = pl.multiple_of(first * bins + part * STEP, STEP)
        return pltpu.make_async_remote_copy(
            src_ref=echo.at[ch, :, pl.ds(start, STEP), :],
            dst_ref=recv.at[slot, me],
            send_sem=z_send.at[slot // units],
            recv_sem=z_recv.at[slot],
            device_id=member(q),
            device_id_type=MESH,
        )

    def own_copy(unit, first, slot):
        ch, part = unit // quads, lax.rem(unit, quads)
        start = pl.multiple_of(first * bins + part * STEP, STEP)
        return pltpu.make_async_copy(
            echo.at[ch, :, pl.ds(start, STEP), :], recv.at[slot, me], z_recv.at[slot]
        )

    def z_landed(slot):
        pltpu.make_async_copy(recv.at[slot], recv.at[slot], z_recv.at[slot]).wait()

    def place(core):
        return rng_size - 1 - core if REVERSE else core

    def send_step(step):
        def to_layer(layer, near):
            for j in range(rng_size):
                q = layer * rng_size + j
                unit = step - LAG * place(j) - FIRST * jnp.minimum(layer, 1)
                valid = (unit >= 0) & (unit < units)
                if near:

                    @pl.when(valid & (rng_i == j))
                    def _():
                        own_copy(unit, me, unit).start()

                    valid = valid & (rng_i != j)

                @pl.when(valid)
                def _():
                    z_copy(unit, q, unit, q).start()

        def send_echo(i, carry):
            for layer in (pulse_i - (depth - 1 - i), pulse_i + depth - 1 - i):

                @pl.when((layer >= 0) & (layer < depth))
                def _(layer=layer):
                    to_layer(layer, False)

            return carry

        lax.fori_loop(0, depth - 1, send_echo, 0)
        to_layer(pulse_i, True)
        early = step - FIRST - RAW
        slot = units + early // quads * halos + lax.rem(early, quads)
        valid = (early >= 0) & (early < units) & (lax.rem(early, quads) < halos)
        if mid > 0:

            @pl.when(valid & (me == mid - 1))
            def _():
                own_copy(early, mid, slot).start()

            @pl.when(valid & (me != mid - 1))
            def _():
                z_copy(early, mid, slot, mid - 1).start()

    mylag = LAG * place(rng_i) + FIRST * jnp.minimum(pulse_i, 1)

    def opening(step, carry):
        send_step(step)
        return carry

    lax.fori_loop(0, AHEAD + mylag, opening, 0)

    def zero_edges():
        @pl.when(me == groups - 1)
        def _():
            spec[:, :, bins:, :, :] = jnp.zeros((chans, 2, SMAX, outer, LANES), BF16)
            quad[:, :, HALF + bins :, :, :] = jnp.zeros((4, 2, HALF, half_rows, LANES), BF16)
            quad_edge[:, :, HALF + bins :, :, :] = jnp.zeros((4, 2, HALF, rows_out, LANES), F32)

        @pl.when(me == 0)
        def _():
            quad[:, :, :HALF, :, :] = jnp.zeros((4, 2, HALF, half_rows, LANES), BF16)
            quad_edge[:, :, :HALF, :, :] = jnp.zeros((4, 2, HALF, rows_out, LANES), F32)

    zero_edges()
    for fetch in fetches:
        fetch.wait()

    per_row = LANES // outer
    for k in range(mig.shape[0]):
        for u in range(outer):
            mig_rows[u : u + 1, :] = mig[k : k + 1, u * LANES : (u + 1) * LANES].astype(F32)
        turned = mig_rows[...].T.astype(BF16)
        total = jnp.zeros((outer, LANES), F32)
        for h in range(per_row):
            total = total + jnp.dot(
                turned[h * outer : (h + 1) * outer],
                slim_t[(2 * two + h * outer) : (2 * two + (h + 1) * outer)],
                preferred_element_type=F32,
            )
        shifts[k] = total.astype(BF16)

    size = outer * LANES
    position = lax.broadcasted_iota(jnp.int32, (outer, LANES), 0) + outer * (
        lax.broadcasted_iota(jnp.int32, (outer, LANES), 1)
    )
    centred = jnp.where(position < size // 2, position, position - size).astype(F32)
    quadratic = centred * centred / size

    def phase_row(r, carry):
        turns = (0.5 * rate[r]) * quadratic
        turns = turns - jnp.round(turns)
        square = turns * turns
        cosine[r] = horner(COS_COEF, square)
        sine[r] = horner(SIN_COEF, square) * turns
        return carry

    lax.fori_loop(0, bins, phase_row, 0)

    def halo_copy(ch, part):
        return pltpu.make_async_remote_copy(
            src_ref=spec.at[ch, :, pl.ds(part * STEP, STEP)],
            dst_ref=spec.at[ch, :, pl.ds(bins + part * STEP, STEP)],
            send_sem=h_send,
            recv_sem=h_recv.at[ch, part],
            device_id=member(jnp.maximum(me - 1, 0)),
            device_id_type=MESH,
        )

    def x_copy(ch, blk, k):
        return pltpu.make_async_remote_copy(
            src_ref=image.at[ch, k - 1, :, pl.ds(blk * STEP, STEP)],
            dst_ref=quad.at[pol_i * chans + ch, :, pl.ds(HALF + blk * STEP, STEP)],
            send_sem=x_send,
            recv_sem=x_recv.at[ch, blk],
            device_id={"pol": lax.rem(pol_i + k, pols)},
            device_id_type=MESH,
        )

    def e_copy(ch, blk, k):
        return pltpu.make_async_remote_copy(
            src_ref=edge.at[ch, k - 1, :, pl.ds(blk * STEP, STEP)],
            dst_ref=quad_edge.at[pol_i * chans + ch, :, pl.ds(HALF + blk * STEP, STEP)],
            send_sem=e_send,
            recv_sem=x_recv.at[ch, blk],
            device_id={"pol": lax.rem(pol_i + k, pols)},
            device_id_type=MESH,
        )

    def drain(array, sem):
        pltpu.make_async_copy(array, array, sem).wait()

    share = 2 * STEP * half_rows // 16 + 2 * STEP * rows_out * 4 // (16 * 2)
    part_row = pl.ds(0, 16)

    def landed(ch, blk):
        if pols > 1:
            drain(quad.at[pl.ds(0, pols - 1), 0, pl.ds(0, share), part_row], x_recv.at[ch, blk])

    def relay(array, sems, recvs, chan, side):
        take = HALF if side == 0 else bins
        put = HALF + bins if side == 0 else 0
        target = jnp.maximum(me - 1, 0) if side == 0 else jnp.minimum(me + 1, groups - 1)
        return pltpu.make_async_remote_copy(
            src_ref=array.at[chan, :, pl.ds(take, HALF)],
            dst_ref=array.at[chan, :, pl.ds(put, HALF)],
            send_sem=sems.at[side],
            recv_sem=recvs.at[side],
            device_id=member(target),
            device_id_type=MESH,
        )

    sides = ((0, me > 0), (1, me < groups - 1))

    def unpack(slot):
        def body(p, carry):
            for part in range(2):
                for a in range(local_a):
                    tile = recv[slot, p, part, :, a * LANES : (a + 1) * LANES].astype(F32)
                    start = pl.multiple_of((part * outer + p * local_a + a) * STEP, STEP)
                    unpacked[pl.ds(start, STEP), :] = tile
            return carry

        lax.fori_loop(0, groups, body, 0)

    def forward(ch, g):
        rows = [unpacked[pl.ds(j, 2 * outer, stride=STEP), :] for j in range(STEP)]
        wide = jnp.concatenate([row.astype(BF16) for row in rows], axis=1)
        half = jnp.dot(first_t[...], wide, preferred_element_type=F32)
        tc, ts = twiddle[0], twiddle[1]
        turned = []
        for j in range(STEP):
            re = half[:outer, j * LANES : (j + 1) * LANES]
            im = half[outer:, j * LANES : (j + 1) * LANES]
            turned.append(
                jnp.concatenate(
                    [(re * tc + im * ts).astype(BF16), (im * tc - re * ts).astype(BF16)], axis=1
                )
            )
        done = jnp.dot(
            jnp.concatenate(turned, axis=0), fwd_t[...], preferred_element_type=F32
        ).astype(BF16)
        for j in range(STEP):
            r = g * STEP + j
            spec[ch, 0, r] = done[j * outer : (j + 1) * outer, :LANES]
            spec[ch, 1, r] = done[j * outer : (j + 1) * outer, LANES:]

    def inverse(ch, blk, g):
        amount = shifts[blk]
        turned = []
        for j in range(STEP):
            r = g * STEP + j
            re, im = spec[ch, 0, r], spec[ch, 1, r]
            for s in range(1, SMAX + 1):
                hit = amount == s
                re = jnp.where(hit, spec[ch, 0, r + s], re)
                im = jnp.where(hit, spec[ch, 1, r + s], im)
            re, im = re.astype(F32), im.astype(F32)
            c, s_ = cosine[r], sine[r]
            turned.append(
                jnp.concatenate(
                    [(re * c - im * s_).astype(BF16), (re * s_ + im * c).astype(BF16)], axis=1
                )
            )
        mid = jnp.dot(jnp.concatenate(turned, axis=0), inv_t[...], preferred_element_type=F32)
        tc, ts = twiddle[2], twiddle[3]
        columns = []
        for j in range(STEP):
            re = mid[j * outer : (j + 1) * outer, :LANES]
            im = mid[j * outer : (j + 1) * outer, LANES:]
            columns.append(
                jnp.concatenate(
                    [(re * tc - im * ts).astype(BF16), (im * tc + re * ts).astype(BF16)], axis=0
                )
            )
        done = jnp.dot(
            last_t[...], jnp.concatenate(columns, axis=1), preferred_element_type=F32
        )
        for j in range(STEP):
            for part in range(2):
                full = done[part * outer : (part + 1) * outer, j * LANES : (j + 1) * LANES]
                r = g * STEP + j
                zero = jnp.zeros((1, LANES), F32)
                rounded = full.astype(BF16)
                exact = rounded.astype(F32)
                pieces = []
                for h in range(pols):
                    low, high = h * half_rows, (h + 1) * half_rows
                    before = exact[low - 1 : low] if h > 0 else zero
                    after = exact[high : high + 1] if h < pols - 1 else zero
                    outside = [before, after]
                    if rows_out == 1:
                        outside = [after if h == 0 else before]
                    pieces.append([exact[low:high]] + outside)
                for k in range(pols):
                    main, *outside = pieces[k]
                    for p in range(1, pols):
                        mine = pol_i == p
                        other = pieces[(p + k) % pols]
                        main = jnp.where(mine, other[0], main)
                        outside = [jnp.where(mine, o, v) for o, v in zip(other[1:], outside)]
                    if k == 0:
                        chan = pol_i * chans + ch
                        quad[chan, part, HALF + r] = main.astype(BF16)
                        for n, row in enumerate(outside):
                            quad_edge[chan, part, HALF + r, n : n + 1] = row
                    else:
                        image[ch, k - 1, part, r] = main.astype(BF16)
                        for n, row in enumerate(outside):
                            edge[ch, k - 1, part, r, n : n + 1] = row

    def loop(count, start, fun):
        def body(i, carry):
            fun(start + i)
            return carry

        lax.fori_loop(0, count, body, 0)

    def pauli(source, target, r):
        v = [[source[c, part, r].astype(F32) for part in range(2)] for c in range(4)]
        k1 = [(v[0][i] + v[3][i]) * ROOT_HALF for i in range(2)]
        k2 = [(v[0][i] - v[3][i]) * ROOT_HALF for i in range(2)]
        k3 = [(v[1][i] + v[2][i]) * ROOT_HALF for i in range(2)]
        terms = [k[0] * k[0] + k[1] * k[1] for k in (k1, k2, k3)]
        for a, b in ((k1, k2), (k1, k3), (k2, k3)):
            terms.append(a[0] * b[0] + a[1] * b[1])
            terms.append(a[1] * b[0] - a[0] * b[1])
        for i, term in enumerate(terms):
            target[i, r] = term

    def cell_row(r):
        pauli(quad, cells, r)
        pauli(quad_edge, cells_edge, r)

    def rim_copies(ch, side, owner):
        @pl.when(sides[side][1])
        def _():
            relay(quad, r_send, r_recv, owner * chans + ch, side).start()
            relay(quad_edge, r_send, r_recv, owner * chans + ch, side).start()

    def pass_on(ch, side):
        landed(ch, rims[side])
        for k in range(side, pols):
            rim_copies(ch, side, lax.rem(pol_i + k, pols))

    def produce(ch, blk):
        inverse(ch, blk * STEP // RBLK, blk)
        for k in range(1, pols):
            e_copy(ch, blk, k).start()
            x_copy(ch, blk, k).start()
        if blk == quads - 1:
            rim_copies(ch, 1, pol_i)

    def take_halo(ch, part):
        @pl.when((me < groups - 1) & (me != mid - 1))
        def _():
            halo_copy(ch, part).wait_recv()

        @pl.when(me == mid - 1)
        def _():
            slot = units + ch * halos + part
            z_landed(slot)
            unpack(slot)
            forward(ch, quads + part)

    rims = (0, quads - 1)
    lagging = place(rng_i) == rng_size - 1
    leading = place(rng_i) != rng_size - 1
    prompt = lagging & (me != mid - 1)
    late = list(range(quads - halos, quads))
    for ch in range(chans):
        for part in range(quads):
            unit = ch * quads + part
            z_landed(unit)
            send_step(unit + AHEAD + mylag)
            unpack(unit)
            forward(ch, part)
            if part < halos:

                @pl.when((me > 0) & (me != mid))
                def _(ch=ch, part=part):
                    halo_copy(ch, part).start()

            if part >= halos and (part < quads - 1 or ch < chans - 1):
                produce(ch, part - halos)
            if part == quads - 1 and ch < chans - 1:

                @pl.when(prompt)
                def _(ch=ch):
                    for h in range(halos):

                        @pl.when(me < groups - 1)
                        def _(h=h):
                            halo_copy(ch, h).wait_recv()

                        produce(ch, late[h])
            if ch > 0:
                if part < halos:

                    @pl.when(jnp.logical_not(prompt))
                    def _(ch=ch, part=part):
                        take_halo(ch - 1, part)
                        produce(ch - 1, late[part])

    def range_sum(x, count):
        two = x[:-1] + x[1:]
        four = two[:-2] + two[2:]
        return four[:count] + two[4 : 4 + count] + x[6 : 6 + count]

    def component(i, low, high):
        slot, count = i % SLOTS, high - low
        tall = slice(low, high + 2 * HALF)
        for j in range(half_rows // 8):
            padded[slot, :count, 8 + j * 8 : 16 + j * 8, :] = range_sum(
                cells[i, tall, j * 8 : (j + 1) * 8, :], count
            )
        rim = range_sum(cells_edge[i, tall], count)
        before, after = rim[:, 0:1, :], rim[:, rows_out - 1 :, :]
        if rows_out == 1:
            before = jnp.where(pol_i == 0, 0.0, before)
            after = jnp.where(pol_i == 0, after, 0.0)
        padded[slot, :count, 7:8, :] = before
        padded[slot, :count, 8 + half_rows : 9 + half_rows, :] = after
        center = padded[slot, :count, 8 : 8 + half_rows, :]
        lane = lax.broadcasted_iota(jnp.int32, (count, half_rows, LANES), 2)
        side = jnp.where(
            lane < LANES // 2,
            padded[slot, :count, 9 : 9 + half_rows, :],
            padded[slot, :count, 7 : 7 + half_rows, :],
        )
        flat = (count * half_rows, LANES)
        both = jnp.concatenate(
            [center.reshape(flat).astype(BF16), side.reshape(flat).astype(BF16)], axis=1
        )
        total = jnp.dot(both, band[...], preferred_element_type=F32)
        total = total * (1.0 / (WIN * WIN))
        for r in range(count):
            start = (low + r) * (half_rows + 8)
            result[i, start : start + half_rows] = total[r * half_rows : (r + 1) * half_rows]

    def gather(i):
        for a in range(half_rows):
            piece = result[i, pl.ds(a, bins, stride=half_rows + 8), :]
            out[i, :, a * LANES : (a + 1) * LANES] = piece.astype(BF16)

    def window(low, high, finish=False):
        for i in range(9):
            component(i, low, high)
            if finish and i > 0:
                gather(i - 1)
        if finish:
            gather(8)

    def take_rim(side):
        @pl.when((me < groups - 1) if side == 0 else (me > 0))
        def _():
            drain(quad.at[pl.ds(0, HALF), 0, pl.ds(0, share), part_row], r_recv.at[side])

        loop(HALF, bins + HALF if side == 0 else 0, cell_row)

    def take_quad(blk):
        landed(last, blk)
        loop(STEP, HALF + blk * STEP, cell_row)

    last = chans - 1
    inner = quads - 1 - halos

    def take_halos():
        for part in range(halos):
            take_halo(last, part)

    produce(last, inner)
    take_halos()
    produce(last, quads - 1)
    for blk in late[:-1]:
        produce(last, blk)
    for ch in range(chans):
        if ch < last:
            for side in range(2):
                pass_on(ch, side)
            for blk in range(1, quads - 1):
                landed(ch, blk)
    pass_on(last, 0)
    loop(STEP, HALF, cell_row)
    early = (quads - halos) * STEP - HALF

    def take_rim_quad():
        pass_on(last, 1)
        loop(STEP, HALF + (quads - 1) * STEP, cell_row)

    @pl.when(lagging)
    def _():
        for blk in range(1, quads - halos):
            take_quad(blk)
        take_rim(1)
        window(0, early)
        take_rim_quad()
        take_rim(0)
        for blk in range(quads - halos, quads - 1):
            take_quad(blk)
        window(early, bins, True)

    @pl.when(leading)
    def _():
        for blk in range(1, quads - halos):
            take_quad(blk)
        take_rim_quad()
        for blk in range(quads - halos, quads - 1):
            take_quad(blk)
        window(HALF, bins - HALF)
        take_rim(0)
        window(bins - HALF, bins)
        take_rim(1)
        window(0, HALF, True)

    drain(recv.at[pl.ds(0, units), pl.ds(0, groups - 1)], z_send.at[0])

    @pl.when(me != mid - 1)
    def _():
        drain(recv.at[pl.ds(0, chans * halos), 0], z_send.at[1])

    @pl.when((me > 0) & (me != mid))
    def _():
        drain(spec.at[:, :, pl.ds(0, SMAX)], h_send)

    if pols > 1:
        drain(image, x_send)
        drain(edge, e_send)
    for side, cond in sides:

        @pl.when(cond)
        def _(side=side):
            drain(quad.at[pl.ds(0, HALF), 0, pl.ds(0, share), part_row], r_send.at[side])


def shards(echoes, migration, fm_rate):
    rng_size = lax.axis_size("rng")
    groups = lax.axis_size("pulse") * rng_size
    pols = lax.axis_size("pol")
    chans = echoes.shape[0]
    pulses = echoes.shape[3]
    bins = echoes.shape[2] // groups
    outer = groups * pulses // LANES
    half_rows = outer // pols
    units = chans * (bins // STEP)
    consts = tables(outer)
    vmem = pl.BlockSpec(memory_space=pltpu.VMEM)
    anywhere = pl.BlockSpec(memory_space=pltpu.HBM)
    dma = pltpu.SemaphoreType.DMA
    tall = bins + 2 * HALF
    return pl.pallas_call(
        functools.partial(kernel, chans, groups, pols, bins, outer, rng_size),
        out_shape=pltpu.VMEM((9, bins, half_rows * LANES), BF16),
        in_specs=[
            anywhere,
            anywhere,
            pl.BlockSpec(memory_space=pltpu.SMEM),
        ]
        + [anywhere] * len(consts),
        out_specs=vmem,
        scratch_shapes=[
            pltpu.VMEM(migration.shape, jnp.int32),
            *(pltpu.VMEM(table.shape, table.dtype) for table in consts),
            dma((1 + len(consts),)),
            pltpu.VMEM((units + chans * (SMAX // STEP), groups, 2, STEP, pulses), BF16),
            pltpu.VMEM((2 * outer * STEP, LANES), F32),
            pltpu.VMEM((chans, 2, bins + SMAX, outer, LANES), BF16),
            pltpu.VMEM((chans, pols - 1, 2, bins, half_rows, LANES), BF16),
            pltpu.VMEM((chans, pols - 1, 2, bins, edge_rows(pols), LANES), F32),
            pltpu.VMEM((4, 2, tall, half_rows, LANES), BF16),
            pltpu.VMEM((4, 2, tall, edge_rows(pols), LANES), F32),
            pltpu.VMEM((migration.shape[0], outer, LANES), BF16),
            pltpu.VMEM((outer, LANES), F32),
            pltpu.VMEM((bins, outer, LANES), F32),
            pltpu.VMEM((bins, outer, LANES), F32),
            pltpu.VMEM((9, tall, half_rows, LANES), F32),
            pltpu.VMEM((9, tall, edge_rows(pols), LANES), F32),
            pltpu.VMEM((SLOTS, bins, half_rows + 16, LANES), F32),
            pltpu.VMEM((9, bins * (half_rows + 8), LANES), F32),
            dma((2,)),
            dma((units + chans * (SMAX // STEP),)),
            dma,
            dma((chans, SMAX // STEP)),
            dma,
            dma((chans, bins // STEP)),
            dma,
            dma((2,)),
            dma((2,)),
        ],
        compiler_params=pltpu.CompilerParams(
            collective_id=0,
            has_side_effects=True,
            vmem_limit_bytes=58 * 1024 * 1024,
        ),
    )(echoes, migration, fm_rate, *consts)


def solution(mesh):
    placed = (
        P(("scene", "pol"), None, None, ("pulse", "rng")),
        P(("scene", "pulse", "rng"), None),
        P(("scene", "pulse", "rng")),
    )
    return jax.shard_map(
        shards,
        mesh=mesh,
        in_specs=placed,
        out_specs=P(None, ("scene", "pulse", "rng"), "pol"),
        check_vma=False,
    )
```
